32 devices in a mesh: groups: 2 (over y), cand: 4 (over z), mp: 4 (over x, core).
Axes of the slice: x: 2, y: 2, z: 4, core: 2. Of those that a mesh axis runs over, the one named last changes fastest.
Arguments:
- user_feats: bfloat16 [8, 4096], P(('groups', 'cand')), parts along dimension 0, may hold values from -6 to 6
- user_slot: int32 [2], P('groups'), parts along dimension 0, may hold values from 0 to 3, as said below
- cand_pool: bfloat16 [512, 4096], P('groups'), parts along dimension 0, may hold values from -6 to 6
- cand_ids: int32 [2, 64], P('groups'), parts along dimension 0, may hold values from 0 to 255
- first_weight: bfloat16 [8192, 8192], P('mp', 'cand'), may hold values from -0.0625 to 0.0625
- first_bias: float32 [8192], P('cand'), may hold values from -5 to 5
- second_weight: bfloat16 [8192, 8192], P('cand', 'mp'), may hold values from -0.0625 to 0.0625
- second_bias: float32 [8192], P('mp'), may hold values from -5 to 5
- third_weight: bfloat16 [8192, 8192], P('mp', 'cand'), may hold values from -0.0625 to 0.0625
- third_bias: float32 [8192], P('cand'), may hold values from -5 to 5
- score_weight: bfloat16 [8192], P('cand'), may hold values from -0.0625 to 0.0625
Outputs:
- crossed: bfloat16 [128, 8192], P(('groups', 'mp'), 'cand'), parts along dimension 0
- logits: float32 [128], P(('groups', 'mp')), parts along dimension 0
The draws below stay inside these ranges and needn't reach their ends.
There are 2 independent parts, one for each index of `groups`. The reference program is written for one: setup_inputs(seed, part) draws one part's arguments, and reference() takes and returns one part's arrays. A program takes and returns all parts, laid end to end along the dimension named above; an argument that names none is the same for every part. Nothing has to cross between parts.
Inputs may be any that keep to these rules, and one draw needn't show every extreme that they name: `user_slot`: the users' slots are distinct.
All inputs are finite; a program needn't handle non-finite values.
Results may differ from the reference program's by a relative error of at most 0.022.
Values may be sent and summed in bfloat16 or wider, within the bound.
A program may use at most 64 MiB of HBM per device.

```python
import jax
import jax.numpy as jnp
from jax import lax

DH = 4096
D = 8192
POOL = 256
CANDS = 64
USERS = 1
SLOTS = 4
ROWS = 64
N_CAND = 4


def draw_user_slot(key, part):
    pairs = jax.random.permutation(jax.random.fold_in(key, 11), SLOTS // 2)[:USERS].astype(jnp.int32)
    bits = jax.random.randint(jax.random.fold_in(key, 12), (USERS,), 0, 2).astype(jnp.int32)
    first_bit = (jnp.asarray(part).astype(jnp.int32) % 2).astype(jnp.int32)
    bits = bits.at[0].set(first_bit)
    return (2 * pairs + bits).astype(jnp.int32)


def with_ends(drawn, key, low, largest):
    longest = drawn.shape.index(max(drawn.shape))
    spots = []
    for shift in (0, 1):
        where = [jax.random.randint(jax.random.fold_in(key, axis), (), 0, length) for axis, length in enumerate(drawn.shape)]
        where[longest] = (where[longest] + shift) % drawn.shape[longest]
        spots.append(tuple(where))
    return drawn.at[spots[0]].set(low).at[spots[1]].set(largest)


def block_scale(rng, dims, split, smallest, largest):
    def one(dim, blocks):
        steps = jax.random.uniform(jax.random.fold_in(jax.random.fold_in(rng, 6), dim), (blocks,), jnp.float32, smallest / len(split), largest / len(split))
        return jnp.repeat(jnp.exp(steps), dims[dim] // blocks).reshape((-1,) + (1,) * (len(dims) - dim - 1))

    level = one(*split[0])
    for cut in split[1:]:
        level = level * one(*cut)
    return level


def gaussian(key, shape, scale, limit, pieces=(), held_as=jnp.bfloat16):
    array = scale * jax.random.normal(key, shape, jnp.float32)
    if pieces:
        array = array * block_scale(key, shape, pieces, -0.22, 0.18)
    return jnp.clip(array, -limit, limit).astype(held_as)


def setup_inputs(seed: int = 0, part: int = 0) -> dict:
    key_list = jax.random.split(jax.random.key(seed), 12)
    part_splits = jax.random.split(jax.random.fold_in(key_list[11], part), 12)
    return {
        "user_feats": gaussian(part_splits[0], (SLOTS, DH), 1.0, 6.0, ((0, 4),)),
        "user_slot": draw_user_slot(jax.random.fold_in(jax.random.fold_in(key_list[11], part), 71), part),
        "cand_pool": gaussian(part_splits[2], (POOL, DH), 1.0, 6.0),
        "cand_ids": with_ends(jax.random.randint(part_splits[3], (USERS, CANDS), 0, POOL), jax.random.fold_in(part_splits[3], 1), 0, POOL - 1).astype(jnp.int32),
        "first_weight": gaussian(key_list[4], (D, D), D ** -0.5, 0.0625, ((0, 4), (1, 4))),
        "first_bias": gaussian(key_list[5], (D,), 1.0, 5.0, ((0, 4),), jnp.float32),
        "second_weight": gaussian(key_list[6], (D, D), D ** -0.5, 0.0625, ((0, 4), (1, 4))),
        "second_bias": gaussian(key_list[7], (D,), 1.0, 5.0, ((0, 4),), jnp.float32),
        "third_weight": gaussian(key_list[8], (D, D), D ** -0.5, 0.0625, ((0, 4), (1, 4))),
        "third_bias": gaussian(key_list[9], (D,), 1.0, 5.0, ((0, 4),), jnp.float32),
        "score_weight": gaussian(key_list[10], (D,), D ** -0.5, 0.0625, ((0, 4),)),
    }


def reference(user_feats, user_slot, cand_pool, cand_ids, first_weight, first_bias, second_weight, second_bias, third_weight, third_bias, score_weight):
    user_rows = jnp.repeat(user_feats[user_slot], CANDS, axis=0)
    pool_rows = cand_pool[cand_ids.reshape(-1)]
    base = jnp.concatenate([user_rows, pool_rows], axis=1)
    first_sum = jnp.dot(base, first_weight, preferred_element_type=jnp.float32)
    cross_one = (base * (first_sum + first_bias) + base).astype(jnp.bfloat16)
    block = D // N_CAND
    second_sum = jnp.zeros((ROWS, D), jnp.float32)
    for piece in range(N_CAND):
        term = jnp.dot(cross_one[:, piece * block:(piece + 1) * block], second_weight[piece * block:(piece + 1) * block], preferred_element_type=jnp.float32)
        term = lax.optimization_barrier(term.astype(jnp.bfloat16))
        second_sum = second_sum + term.astype(jnp.float32)
    cross_two = (base * (second_sum + second_bias) + cross_one).astype(jnp.bfloat16)
    third_sum = jnp.dot(cross_two, third_weight, preferred_element_type=jnp.float32)
    cross_three = base * (third_sum + third_bias) + cross_two
    logits = jnp.sum(cross_three * score_weight.astype(jnp.float32), axis=1)
    return cross_three.astype(jnp.bfloat16), logits
```

```python
import contextlib

import jax
import jax.numpy as jnp
from jax import lax
from jax.experimental import pallas as pl
from jax.experimental.pallas import tpu as pltpu
from jax.sharding import PartitionSpec as P

MESH = pl.DeviceIdType.MESH
F32 = jnp.float32
BF16 = jnp.bfloat16


def scope(name):
    return contextlib.nullcontext()


def reverse_bits(value, bits):
    out = 0
    for _ in range(bits):
        out = 2 * out + value % 2
        value = value // 2
    return out


def hand_on(crossed_ref, logit_ref, crossed_hbm, logit_hbm, sem):
    copies = [
        pltpu.make_async_copy(crossed_ref, crossed_hbm, sem.at[0]),
        pltpu.make_async_copy(logit_ref, logit_hbm, sem.at[1]),
    ]
    for copy in copies:
        copy.start()
    for copy in copies:
        copy.wait()


def make_kernel(n_mp, n_cand, shapes):
    rows, per_user, users, slots_each, half_width, pool_count, feat, col, n1, n2, n3, lhs_rows = shapes
    cw1, cw2, cw3 = col // n1, feat // n2, col // n3
    bits = n_mp.bit_length() - 1
    low = bits - 1
    half = n_mp // 2
    block = rows // n_mp
    ratio = feat // col
    group = n_mp * n_cand
    part = rows // 2
    first_pool_col = half_width // col

    def user_of(p):
        return (reverse_bits(p, bits) * block) // per_user

    def kernel(
        user_hbm, slot_hbm, pool_hbm, ids_hbm, w1_hbm, b1_hbm, w2_hbm, b2_hbm, w3_hbm, b3_hbm, score_hbm,
        out_ref, logit_ref,
        slot_ref, user_ref, ids_ref, b1_ref, b2_ref, b3_ref, score_ref, small_sem, slots, pool_m, pool_c, w1_v, w2_v, w3_v,
        onehot, base_mp, base_col, lhs, acc1, send1, recv1, psum, ubuf, cross1, acc2, q_send, zr, zs, x3, acc3, send3, recv3,
        q_rows, q_all,
        w_sem, user_ss, user_rs, a_ss, a_rs, x_ss, x_rs, g_ss, g_rs, u_ss, u_rs, z_ss, z_rs, c_ss, c_rs, q_ss, q_rs,
    ):
        i = lax.axis_index("mp")
        j = lax.axis_index("cand")
        me = i * n_cand + j
        pending = []
        user_side = i < half
        pool_side = jnp.logical_not(user_side)

        def remote(src, dst, ss, rs, where):
            return pltpu.make_async_remote_copy(
                src_ref=src, dst_ref=dst, send_sem=ss, recv_sem=rs, device_id=where, device_id_type=MESH
            )

        barrier = pltpu.get_barrier_semaphore()
        with scope("greet"):
            def greet(d, carry):
                pl.semaphore_signal(barrier, inc=1, device_id={"cand": lax.rem(j + d, n_cand)}, device_id_type=MESH)
                return carry

            lax.fori_loop(1, n_cand, greet, 0, unroll=n_cand <= 4)
            for d in range(1, n_mp):
                pl.semaphore_signal(barrier, inc=1, device_id={"mp": lax.rem(i + d, n_mp)}, device_id_type=MESH)

        small_copies = [
            pltpu.make_async_copy(src, dst, small_sem.at[k])
            for k, (src, dst) in enumerate(
                (
                    (user_hbm, user_ref), (ids_hbm, ids_ref), (slot_hbm, slot_ref), (b1_hbm, b1_ref),
                    (b2_hbm, b2_ref), (b3_hbm, b3_ref), (score_hbm, score_ref),
                )
            )
        ]
        m_start = pl.multiple_of(jnp.maximum(i - half, 0) * feat, 128)
        c_start = pl.multiple_of(jnp.maximum(j - first_pool_col, 0) * col, 128)
        pool_m_copy = pltpu.make_async_copy(pool_hbm.at[:, pl.ds(m_start, feat)], pool_m, w_sem.at[0])
        pool_c_copy = pltpu.make_async_copy(pool_hbm.at[:, pl.ds(c_start, col)], pool_c, w_sem.at[1])
        w1_copies = [
            pltpu.make_async_copy(w1_hbm.at[:, pl.ds(c * cw1, cw1)], w1_v.at[c], w_sem.at[2 + c]) for c in range(n1)
        ]
        w2_copies = [
            pltpu.make_async_copy(w2_hbm.at[pl.ds(c * cw1, cw1), :], w2_v.at[pl.ds(c * cw1, cw1), :], w_sem.at[2 + n1 + c])
            for c in range(n1)
        ]
        w3_copies = [
            pltpu.make_async_copy(w3_hbm.at[pl.ds(c * cw2, cw2), :], w3_v.at[pl.ds(c * cw2, cw2), :], w_sem.at[2 + 2 * n1 + c])
            for c in range(n2)
        ]
        col_pool = j >= first_pool_col
        with scope("loads"):
            for copy in small_copies[:3]:
                copy.start()

            @pl.when(pool_side)
            def _():
                pool_m_copy.start()

            for copy in w1_copies:
                copy.start()
            for copy in small_copies[3:]:
                copy.start()

            @pl.when(col_pool)
            def _():
                pool_c_copy.start()

            end = jnp.logical_or(j == 0, j == n_cand - 1)
            inner = jnp.logical_not(end)
            nd = (j >= (n_cand + 1) // 2).astype(jnp.int32)

            @pl.when(end)
            def _():
                zr[nd] = jnp.zeros(zr.shape[1:], BF16)

        with scope("onehot"):
            small_copies[1].wait()
            for u in range(users):
                hot = (
                    lax.broadcasted_iota(jnp.int32, (pool_count, per_user), 0) == ids_ref[u : u + 1, :]
                ).astype(F32).T
                for p in range(n_mp):
                    first = reverse_bits(p, bits) * block
                    if first // per_user == u:
                        off = first % per_user
                        onehot[p * block : (p + 1) * block, :] = hot[off : off + block].astype(BF16)

        def from_pool(dst, src, width):
            for c in range(0, width, 256):
                dst[:, c : c + 256] = jnp.dot(onehot[...], src[:, c : c + 256], preferred_element_type=F32).astype(BF16)

        def user_row(u, index, width):
            start = pl.multiple_of(index * width, 128)
            slot = slot_ref[u]
            row = slots[slot // slots_each, :, pl.ds(start, width)].astype(F32)
            if slots_each > 1:
                pick = lax.broadcasted_iota(jnp.int32, row.shape, 0) == lax.rem(slot, slots_each)
                row = jnp.sum(jnp.where(pick, row, 0.0), axis=0, keepdims=True)
            return row

        def from_user(dst, index, width):
            rows_of = [user_row(u, index, width) for u in range(users)]
            for p in range(n_mp):
                dst[p * block : (p + 1) * block, :] = jnp.broadcast_to(rows_of[user_of(p)], (block, width)).astype(BF16)

        def user_copy(d):
            return remote(user_ref, slots.at[j], user_ss.at[d - 1], user_rs.at[j], {"cand": lax.rem(j + d, n_cand)})

        def from_all_users():
            for d in range(1, n_cand):
                k = lax.rem(j - d + n_cand, n_cand)
                remote(user_ref, slots.at[k], user_ss.at[d - 1], user_rs.at[k], {"cand": k}).wait_recv()
            small_copies[2].wait()

        def bit_of(b):
            return lax.rem(i // (1 << b), 2)

        def partner(b):
            return i + (1 << b) * (1 - 2 * bit_of(b))

        lows = [0]
        for b in range(bits):
            lows.append(lows[b] + bit_of(b) * (rows >> (b + 1)))

        def seg(b):
            size = rows >> b
            if b == 0:
                return pl.ds(0, rows)
            return pl.ds(pl.multiple_of(lows[b], size), size)

        def other(b):
            size = rows >> (b + 1)
            start = lows[b] + (1 - bit_of(b)) * size
            return pl.ds(pl.multiple_of(start, size), size)

        def scatter_copy(c, b):
            size = rows >> (b + 1)
            return remote(
                send1.at[c, other(b), :], recv1.at[b, c, pl.ds(0, size), :], a_ss.at[b, c], a_rs.at[b, c], {"mp": partner(b)}
            )

        def across_copy(c):
            return remote(
                psum.at[c, seg(low), :], psum.at[c, seg(low), :], x_ss.at[c], x_rs.at[c], {"mp": lax.rem(i + half, n_mp)}
            )

        def gather_copy(c, b):
            return remote(
                psum.at[c, seg(b + 1), :], psum.at[c, seg(b + 1), :], g_ss.at[b, c], g_rs.at[b, c], {"mp": partner(b)}
            )

        def gather_wait(c, b):
            remote(
                psum.at[c, other(b), :], psum.at[c, other(b), :], g_ss.at[b, c], g_rs.at[b, c], {"mp": partner(b)}
            ).wait_recv()

        def spread(c):
            if low > 0:
                gather_copy(c, low - 1).start()

        def stage_a(c):
            w1_copies[c].wait()
            term = jnp.dot(base_mp[...], w1_v[c], preferred_element_type=F32)
            if low > 0:
                acc1[c] = term
                send1[c] = term.astype(BF16)
            else:
                psum[c] = term.astype(BF16)

        def stage_b(c):
            for b in range(low):
                scatter_copy(c, b).wait_recv()
                size = rows >> (b + 1)
                term = acc1[c, seg(b + 1), :] + recv1[b, c, 0:size, :].astype(F32)
                if b + 1 < low:
                    acc1[c, seg(b + 1), :] = term
                    send1[c, seg(b + 1), :] = term.astype(BF16)
                    scatter_copy(c, b + 1).start()
                else:
                    psum[c, seg(low), :] = term.astype(BF16)
            across_copy(c).start()
            spread(c)

        def part_copy(c, d):
            return remote(ubuf.at[i, c], ubuf.at[i, c], u_ss.at[d, c], u_rs.at[i, c], {"mp": lax.rem(i + d, n_mp)})

        def part_wait(c, src):
            remote(ubuf.at[src, c], ubuf.at[src, c], u_ss.at[0, c], u_rs.at[src, c], {"mp": src}).wait_recv()

        def meet():
            with scope("barrier"):
                small_copies[0].wait()
                pl.semaphore_wait(barrier, n_cand - 1 + n_mp - 1)
            for d in range(1, n_cand):
                user_copy(d).start()
            slots[j] = user_ref[...]

        with scope("firstpart"):
            @pl.when(pool_side)
            def _():
                pool_m_copy.wait()
                from_pool(base_mp, pool_m, feat)
                stage_a(0)

        meet()

        with scope("layer1"):
            @pl.when(pool_side)
            def _():
                if low > 0:
                    scatter_copy(0, 0).start()
                for c in range(1, n1):
                    with scope(f"a{c}"):
                        stage_a(c)
                        if low > 0:
                            scatter_copy(c, 0).start()
                    with scope(f"b{c - 1}"):
                        stage_b(c - 1)
                with scope(f"b{n1 - 1}"):
                    stage_b(n1 - 1)

            @pl.when(user_side)
            def _():
                with scope("users"):
                    from_all_users()
                with scope("lhs"):
                    rows_of = [user_row(u, i, feat) for u in range(users)]
                    if users == 1:
                        lhs[...] = jnp.broadcast_to(rows_of[0], lhs.shape).astype(BF16)
                    else:
                        place = lax.broadcasted_iota(jnp.int32, lhs.shape, 0)
                        filled = jnp.zeros(lhs.shape, F32)
                        for u in range(users):
                            filled = jnp.where(place == u, rows_of[u], filled)
                        lhs[...] = filled.astype(BF16)
                for c in range(n1):
                    with scope(f"um{c}"):
                        w1_copies[c].wait()
                        term = jnp.dot(lhs[...], w1_v[c], preferred_element_type=F32)
                        ubuf[i, c] = term[0:users]
                        for d in range(1, n_mp):
                            part_copy(c, d).start()

        with scope("bases"):
            for copy in w2_copies:
                copy.start()

            @pl.when(pool_side)
            def _():
                from_all_users()

            @pl.when(user_side)
            def _():
                from_user(base_mp, i, feat)

            @pl.when(col_pool)
            def _():
                pool_c_copy.wait()
                from_pool(base_col, pool_c, col)

            @pl.when(jnp.logical_not(col_pool))
            def _():
                from_user(base_col, j, col)

            for copy in small_copies[3:]:
                copy.wait()

        def take_across(c):
            @pl.when(user_side)
            def _():
                with scope(f"across{c}"):
                    across_copy(c).wait_recv()
                spread(c)

        def first_cross(c):
            with scope(f"gw{c}"):
                for b in range(low - 1, -1, -1):
                    gather_wait(c, b)
                    if b > 0:
                        gather_copy(c, b - 1).start()
            with scope(f"pw{c}"):
                @pl.when(user_side)
                def _():
                    for d in range(1, half):
                        part_wait(c, lax.rem(i + d, half))

                @pl.when(pool_side)
                def _():
                    for src in range(half):
                        part_wait(c, src)

            cols = slice(c * cw1, (c + 1) * cw1)
            added = b1_ref[:, cols]
            for src in range(half):
                added = added + ubuf[src, c]
            for p in range(n_mp):
                r = slice(p * block, (p + 1) * block)
                u = user_of(p)
                base = base_col[r, cols].astype(F32)
                cross1[c, r, :] = (base * (psum[c, r, :].astype(F32) + added[u : u + 1]) + base).astype(BF16)

        halves = [slice(g * part, (g + 1) * part) for g in range(2)]
        toward = 1 - 2 * nd

        def z_copy(g, n, way, src, step):
            return remote(
                src.at[n, halves[g], :], zr.at[way, n, halves[g], :], z_ss.at[way, g, n], z_rs.at[way, g, n],
                {"cand": j + step},
            )

        def z_wait(g, n, way):
            remote(
                q_send.at[n, halves[g], :], zr.at[way, n, halves[g], :], z_ss.at[way, g, n], z_rs.at[way, g, n], {"cand": j}
            ).wait_recv()

        def first_out(n):
            cols = slice(n * cw2, (n + 1) * cw2)
            term = jnp.dot(cross1[n1 - 1], w2_v[(n1 - 1) * cw1 : n1 * cw1, cols], preferred_element_type=F32)
            if n1 > 1:
                term = acc2[:, cols] + term
            owner = (j == i * ratio + (n * cw2) // col).astype(F32)
            inside = (n * cw2) % col
            carried = cross1[inside // cw1, :, inside % cw1 : inside % cw1 + cw2].astype(F32)
            term = base_mp[:, cols].astype(F32) * (term + owner * b2_ref[:, cols]) + owner * carried
            q_send[n] = term.astype(BF16)

        ahead = min(3, n1)
        for c in range(ahead):
            take_across(c)
        for c in range(n1):
            first_cross(c)
            if c == 0:
                for copy in w3_copies:
                    copy.start()
            if c + ahead < n1:
                take_across(c + ahead)
            w2_copies[c].wait()
            if c < n1 - 1:
                with scope(f"l2_{c}"):
                    term = jnp.dot(cross1[c], w2_v[c * cw1 : (c + 1) * cw1, :], preferred_element_type=F32)
                    acc2[...] = term if c == 0 else acc2[...] + term
        per = min(2, n2)
        for s in range(0, n2, per):
            with scope(f"q{s}"):
                for n in range(s, min(s + per, n2)):
                    first_out(n)

                @pl.when(end)
                def _():
                    for n in range(s, min(s + per, n2)):
                        z_copy(0, n, nd, q_send, toward).start()

        @pl.when(end)
        def _():
            for n in range(n2):
                z_copy(1, n, nd, q_send, toward).start()

        def near(g, n):
            @pl.when(inner)
            def _():
                with scope(f"near{g}_{n}"):
                    z_wait(g, n, nd)
                zs[nd, n, halves[g], :] = (zr[nd, n, halves[g], :].astype(F32) + q_send[n, halves[g], :].astype(F32)).astype(BF16)
                z_copy(g, n, nd, zs.at[nd], toward).start()

        def far(g, n):
            with scope(f"far{g}_{n}"):
                z_wait(g, n, 1 - nd)

            @pl.when(inner)
            def _():
                zs[1 - nd, n, halves[g], :] = (
                    zr[1 - nd, n, halves[g], :].astype(F32) + q_send[n, halves[g], :].astype(F32)
                ).astype(BF16)
                z_copy(g, n, 1 - nd, zs.at[1 - nd], -toward).start()

        def third(g, n):
            cols = slice(n * cw2, (n + 1) * cw2)
            r = halves[g]
            value = (
                q_send[n, r, :].astype(F32) + zr[0, n, r, :].astype(F32) + zr[1, n, r, :].astype(F32)
            ).astype(BF16)
            x3[r, cols] = value
            if g == 0:
                w3_copies[n].wait()
            term = jnp.dot(value, w3_v[cols, :], preferred_element_type=F32)
            acc3[r, :] = term if n == 0 else acc3[r, :] + term

        def own_start(d):
            peer = lax.rem(i + d, n_mp)
            return peer, pl.ds(pl.multiple_of(reverse_bits(peer, bits) * block, block), block)

        def last_copy(c, d):
            peer, r = own_start(d)
            cols = slice(c * cw3, (c + 1) * cw3)
            return remote(
                send3.at[r, cols], recv3.at[i, :, cols], c_ss.at[d, c], c_rs.at[i, c], {"mp": peer}
            )

        owner3 = (i == j // ratio).astype(F32)

        def epilogue(g):
            r = halves[g]
            same = bit_of(0) == g
            lanes = jnp.zeros((part, 128), F32)
            for c in range(n3):
                cols = slice(c * cw3, (c + 1) * cw3)
                if ratio == 1:
                    carried = x3[r, cols]
                else:
                    carried = x3[r, pl.ds(pl.multiple_of(lax.rem(j, ratio) * col + c * cw3, 128), cw3)]
                term = (
                    base_col[r, cols].astype(F32) * (acc3[r, cols] + owner3 * b3_ref[:, cols])
                    + owner3 * carried.astype(F32)
                )
                acc3[r, cols] = term
                send3[r, cols] = term.astype(BF16)

                @pl.when(same)
                def _():
                    for d in range(2, n_mp, 2):
                        last_copy(c, d).start()

                @pl.when(jnp.logical_not(same))
                def _():
                    for d in range(1, n_mp, 2):
                        last_copy(c, d).start()

            for c in range(n3):
                cols = slice(c * cw3, (c + 1) * cw3)
                scored = acc3[r, cols] * score_ref[cols].astype(F32).reshape(1, cw3)
                for k in range(0, cw3, 128):
                    lanes = lanes + scored[:, k : k + 128]
            q_rows[r, :] = lanes

        events = [(g, n) for g in range(2) for n in range(n2)]
        skew = min(8, n2)
        if max(rows, 128) > rows:
            q_rows[rows:, :] = jnp.zeros((max(rows, 128) - rows, 128), F32)
        for s in range(len(events) + skew):
            if s < len(events):
                near(*events[s])
            if s < skew:
                continue
            g, n = events[s - skew]
            far(g, n)
            with scope(f"third{g}_{n}"):
                third(g, n)
            if n == n2 - 1:
                with scope(f"epi{g}"):
                    epilogue(g)

        with scope("qsend"):
            q_all[me] = jnp.sum(q_rows[...].T, axis=0, keepdims=True)

            def q_copy(d):
                peer = lax.rem(me + d, group)
                return remote(
                    q_all.at[me], q_all.at[me], q_ss.at[d], q_rs.at[me],
                    {"mp": peer // n_cand, "cand": lax.rem(peer, n_cand)},
                )

            def q_start(d, carry):
                q_copy(d).start()
                return carry

            lax.fori_loop(1, group, q_start, 0)

        mine = pl.ds(pl.multiple_of(reverse_bits(i, bits) * block, block), block)
        for c in range(n3):
            cols = slice(c * cw3, (c + 1) * cw3)
            with scope(f"last{c}"):
                for d in range(1, n_mp):
                    src = lax.rem(i - d + n_mp, n_mp)
                    remote(
                        send3.at[mine, cols], recv3.at[src, :, cols], c_ss.at[d, c], c_rs.at[src, c], {"mp": src}
                    ).wait_recv()
            term = acc3[mine, cols]
            for d in range(1, n_mp):
                term = term + recv3[lax.rem(i - d + n_mp, n_mp), :, cols].astype(F32)
            out_ref[:, cols] = term.astype(BF16)

        with scope("qwait"):
            def q_wait(d, carry):
                k = lax.rem(me - d + group, group)
                remote(q_all.at[k], q_all.at[k], q_ss.at[d], q_rs.at[k], {"cand": j}).wait_recv()
                return carry

            lax.fori_loop(1, group, q_wait, 0)
            total = jnp.sum(q_all[...], axis=0)
            for k in range(n_mp):
                p = reverse_bits(k, bits)

                @pl.when(i == k)
                def _():
                    logit_ref[...] = total[:, p * block : (p + 1) * block]

        with scope("sent"):
            for d in range(1, n_cand):
                user_copy(d).wait_send()
            for c in range(n1):
                @pl.when(pool_side)
                def _():
                    for b in range(low):
                        scatter_copy(c, b).wait_send()
                    across_copy(c).wait_send()

                @pl.when(user_side)
                def _():
                    for d in range(1, n_mp):
                        part_copy(c, d).wait_send()

                for b in range(low):
                    gather_copy(c, b).wait_send()
            for g in range(2):
                for n in range(n2):
                    z_copy(g, n, nd, q_send, toward).wait_send()

                    @pl.when(inner)
                    def _():
                        z_copy(g, n, 1 - nd, q_send, -toward).wait_send()
            for c in range(n3):
                for d in range(1, n_mp):
                    last_copy(c, d).wait_send()

            def q_sent(d, carry):
                q_copy(d).wait_send()
                return carry

            lax.fori_loop(1, group, q_sent, 0)

    return kernel


def solution(mesh):
    n_mp, n_cand = mesh.shape["mp"], mesh.shape["cand"]

    def body(
        user_feats, user_slot, cand_pool, cand_ids, first_weight, first_bias,
        second_weight, second_bias, third_weight, third_bias, score_weight,
    ):
        slots_each, half_width = user_feats.shape
        users, per_user = cand_ids.shape
        rows = users * per_user
        pool_count = cand_pool.shape[0]
        feat, col = first_weight.shape
        n1 = max(1, col // 256)
        n2 = max(1, feat // 256)
        n3 = max(1, col // 512)
        lhs_rows = -(-users // 16) * 16
        cw1, cw2 = col // n1, feat // n2
        bits = n_mp.bit_length() - 1
        low = max(1, bits - 1)
        half = n_mp // 2
        block = rows // n_mp
        group = n_mp * n_cand
        shapes = (rows, per_user, users, slots_each, half_width, pool_count, feat, col, n1, n2, n3, lhs_rows)
        vmem = pl.BlockSpec(memory_space=pltpu.VMEM)
        hbm = pl.BlockSpec(memory_space=pl.ANY)
        dma = pltpu.SemaphoreType.DMA
        crossed, logits = pl.pallas_call(
            make_kernel(n_mp, n_cand, shapes),
            out_shape=(
                pltpu.VMEM((block, col), BF16),
                pltpu.VMEM((1, block), F32),
            ),
            in_specs=[hbm] * 11,
            out_specs=(vmem, vmem),
            scratch_shapes=[
                pltpu.SMEM((users,), jnp.int32),
                pltpu.VMEM((slots_each, half_width), BF16),
                pltpu.VMEM((users, per_user), jnp.int32),
                pltpu.VMEM((1, col), F32),
                pltpu.VMEM((1, feat), F32),
                pltpu.VMEM((1, col), F32),
                pltpu.VMEM((col,), BF16),
                dma((7,)),
                pltpu.VMEM((n_cand, slots_each, half_width), BF16),
                pltpu.VMEM((pool_count, feat), BF16),
                pltpu.VMEM((pool_count, col), BF16),
                pltpu.VMEM((n1, feat, cw1), BF16),
                pltpu.VMEM((col, feat), BF16),
                pltpu.VMEM((feat, col), BF16),
                pltpu.VMEM((rows, pool_count), BF16),
                pltpu.VMEM((rows, feat), BF16),
                pltpu.VMEM((rows, col), BF16),
                pltpu.VMEM((lhs_rows, feat), BF16),
                pltpu.VMEM((n1, rows, cw1), F32),
                pltpu.VMEM((n1, rows, cw1), BF16),
                pltpu.VMEM((low, n1, rows // 2, cw1), BF16),
                pltpu.VMEM((n1, rows, cw1), BF16),
                pltpu.VMEM((half, n1, users, cw1), F32),
                pltpu.VMEM((n1, rows, cw1), BF16),
                pltpu.VMEM((rows, feat), F32),
                pltpu.VMEM((n2, rows, cw2), BF16),
                pltpu.VMEM((2, n2, rows, cw2), BF16),
                pltpu.VMEM((2, n2, rows, cw2), BF16),
                pltpu.VMEM((rows, feat), BF16),
                pltpu.VMEM((rows, col), F32),
                pltpu.VMEM((rows, col), BF16),
                pltpu.VMEM((n_mp, block, col), BF16),
                pltpu.VMEM((max(rows, 128), 128), F32),
                pltpu.VMEM((group, 1, max(rows, 128)), F32),
                dma((2 + 2 * n1 + n2,)),
                dma((n_cand,)),
                dma((n_cand,)),
                dma((low, n1)),
                dma((low, n1)),
                dma((n1,)),
                dma((n1,)),
                dma((low, n1)),
                dma((low, n1)),
                dma((n_mp, n1)),
                dma((half, n1)),
                dma((2, 2, n2)),
                dma((2, 2, n2)),
                dma((n_mp, n3)),
                dma((n_mp, n3)),
                dma((group,)),
                dma((group,)),
            ],
            compiler_params=pltpu.CompilerParams(
                collective_id=0, has_side_effects=True, vmem_limit_bytes=67043328 - 3000 * 1024
            ),
        )(
            user_feats, user_slot, cand_pool, cand_ids, first_weight, first_bias.reshape(1, -1),
            second_weight, second_bias.reshape(1, -1), third_weight, third_bias.reshape(1, -1),
            score_weight,
        )
        crossed, logits = pl.pallas_call(
            hand_on,
            out_shape=(
                jax.ShapeDtypeStruct((block, col), BF16),
                jax.ShapeDtypeStruct((1, block), F32),
            ),
            in_specs=[vmem, vmem],
            out_specs=(hbm, hbm),
            scratch_shapes=[dma((2,))],
            compiler_params=pltpu.CompilerParams(vmem_limit_bytes=1024 * 1024),
        )(crossed, logits)
        return crossed, logits.reshape(-1)

    in_specs = (
        P(("groups", "cand"), None),
        P("groups"),
        P("groups", None),
        P("groups", None),
        P("mp", "cand"),
        P("cand"),
        P("cand", "mp"),
        P("mp"),
        P("mp", "cand"),
        P("cand"),
        P("cand"),
    )
    out_specs = (P(("groups", "mp"), "cand"), P(("groups", "mp")))
    return jax.shard_map(body, mesh=mesh, in_specs=in_specs, out_specs=out_specs, check_vma=False)
```

```python
import contextlib

import jax
import jax.numpy as jnp
from jax import lax
from jax.experimental import pallas as pl
from jax.experimental.pallas import tpu as pltpu
from jax.sharding import PartitionSpec as P

MESH = pl.DeviceIdType.MESH
F32 = jnp.float32
BF16 = jnp.bfloat16


def scope(name):
    return contextlib.nullcontext()


def reverse_bits(value, bits):
    out = 0
    for _ in range(bits):
        out = 2 * out + value % 2
        value = value // 2
    return out


def hand_on(crossed_ref, logit_ref, crossed_hbm, logit_hbm, sem):
    copies = [
        pltpu.make_async_copy(crossed_ref, crossed_hbm, sem.at[0]),
        pltpu.make_async_copy(logit_ref, logit_hbm, sem.at[1]),
    ]
    for copy in copies:
        copy.start()
    for copy in copies:
        copy.wait()


def make_kernel(n_mp, n_cand, shapes):
    rows, per_user, users, slots_each, half_width, pool_count, feat, col, n1, n2, n3, lhs_rows = shapes
    cw1, cw2, cw3 = col // n1, feat // n2, col // n3
    bits = n_mp.bit_length() - 1
    low = bits - 1
    half = n_mp // 2
    block = rows // n_mp
    ratio = feat // col
    group = n_mp * n_cand
    part = rows // 2
    first_pool_col = half_width // col

    def user_of(p):
        return (reverse_bits(p, bits) * block) // per_user

    def kernel(
        user_hbm, slot_hbm, pool_hbm, ids_hbm, w1_hbm, b1_hbm, w2_hbm, b2_hbm, w3_hbm, b3_hbm, score_hbm,
        out_ref, logit_ref,
        slot_ref, ids_ref, b1_ref, b2_ref, b3_ref, score_ref, small_sem, slots, pool_m, pool_c, w1_v, w2_v, w3_v,
        onehot, base_mp, base_col, lhs, acc1, send1, recv1, psum, ubuf, cross1, acc2, q_send, zr, zs, x3, acc3, send3, recv3,
        q_rows, q_all,
        w_sem, user_sem, a_ss, a_rs, x_ss, x_rs, g_ss, g_rs, u_ss, u_rs, z_ss, z_rs, c_ss, c_rs, q_sem,
    ):
        i = lax.axis_index("mp")
        j = lax.axis_index("cand")
        me = i * n_cand + j
        user_side = i < half
        pool_side = jnp.logical_not(user_side)

        def remote(src, dst, ss, rs, where):
            return pltpu.make_async_remote_copy(
                src_ref=src, dst_ref=dst, send_sem=ss, recv_sem=rs, device_id=where, device_id_type=MESH
            )

        barrier = pltpu.get_barrier_semaphore()
        with scope("greet"):
            def greet(d, carry):
                pl.semaphore_signal(barrier, inc=1, device_id={"cand": lax.rem(j + d, n_cand)}, device_id_type=MESH)
                return carry

            lax.fori_loop(1, n_cand, greet, 0, unroll=n_cand <= 4)
            for d in range(1, n_mp):
                pl.semaphore_signal(barrier, inc=1, device_id={"mp": lax.rem(i + d, n_mp)}, device_id_type=MESH)

        small_copies = [
            pltpu.make_async_copy(src, dst, small_sem.at[k])
            for k, (src, dst) in enumerate(
                (
                    (ids_hbm, ids_ref), (slot_hbm, slot_ref), (user_hbm, slots.at[j]), (b1_hbm, b1_ref),
                    (b2_hbm, b2_ref), (b3_hbm, b3_ref), (score_hbm, score_ref),
                )
            )
        ]
        m_start = pl.multiple_of(jnp.maximum(i - half, 0) * feat, 128)
        c_start = pl.multiple_of(jnp.maximum(j - first_pool_col, 0) * col, 128)
        pool_m_copy = pltpu.make_async_copy(pool_hbm.at[:, pl.ds(m_start, feat)], pool_m, w_sem.at[0])
        pool_c_copy = pltpu.make_async_copy(pool_hbm.at[:, pl.ds(c_start, col)], pool_c, w_sem.at[1])
        w1_copies = [
            pltpu.make_async_copy(w1_hbm.at[:, pl.ds(c * cw1, cw1)], w1_v.at[c], w_sem.at[2 + c]) for c in range(n1)
        ]
        w2_copy = pltpu.make_async_copy(w2_hbm, w2_v, w_sem.at[2 + n1])
        w3_copy = pltpu.make_async_copy(w3_hbm, w3_v, w_sem.at[3 + n1])
        col_pool = j >= first_pool_col
        with scope("loads"):
            for copy in small_copies[:3]:
                copy.start()

            @pl.when(pool_side)
            def _():
                pool_m_copy.start()

            for copy in w1_copies:
                copy.start()
            for copy in small_copies[3:]:
                copy.start()

            @pl.when(col_pool)
            def _():
                pool_c_copy.start()

            @pl.when(user_side)
            def _():
                w2_copy.start()

            end = jnp.logical_or(j == 0, j == n_cand - 1)
            inner = jnp.logical_not(end)
            nd = (j >= (n_cand + 1) // 2).astype(jnp.int32)

            @pl.when(end)
            def _():
                zr[nd] = jnp.zeros(zr.shape[1:], BF16)

        def build_onehot():
            with scope("onehot"):
                small_copies[0].wait()
                for u in range(users):
                    hot = (
                        lax.broadcasted_iota(jnp.int32, (pool_count, per_user), 0) == ids_ref[u : u + 1, :]
                    ).astype(F32).T
                    for p in range(n_mp):
                        first = reverse_bits(p, bits) * block
                        if first // per_user == u:
                            off = first % per_user
                            onehot[p * block : (p + 1) * block, :] = hot[off : off + block].astype(BF16)

        def from_pool(dst, src, width):
            for c in range(0, width, 256):
                dst[:, c : c + 256] = jnp.dot(onehot[...], src[:, c : c + 256], preferred_element_type=F32).astype(BF16)

        def user_row(u, index, width):
            start = pl.multiple_of(index * width, 128)
            slot = slot_ref[0, u]
            row = slots[slot // slots_each, :, pl.ds(start, width)].astype(F32)
            if slots_each > 1:
                pick = lax.broadcasted_iota(jnp.int32, row.shape, 0) == lax.rem(slot, slots_each)
                row = jnp.sum(jnp.where(pick, row, 0.0), axis=0, keepdims=True)
            return row

        def from_user(dst, index, width):
            rows_of = [user_row(u, index, width) for u in range(users)]
            for p in range(n_mp):
                dst[p * block : (p + 1) * block, :] = jnp.broadcast_to(rows_of[user_of(p)], (block, width)).astype(BF16)

        def user_copy(d):
            return remote(user_hbm, slots.at[j], user_sem.at[0], user_sem.at[1], {"cand": lax.rem(j + d, n_cand)})

        others = slots.at[pl.ds(0, n_cand - 1)]

        def from_all_users():
            remote(others, others, user_sem.at[0], user_sem.at[1], {"cand": j}).wait_recv()
            small_copies[1].wait()
            small_copies[2].wait()

        def bit_of(b):
            return lax.rem(i // (1 << b), 2)

        def partner(b):
            return i + (1 << b) * (1 - 2 * bit_of(b))

        lows = [0]
        for b in range(bits):
            lows.append(lows[b] + bit_of(b) * (rows >> (b + 1)))

        def seg(b):
            size = rows >> b
            if b == 0:
                return pl.ds(0, rows)
            return pl.ds(pl.multiple_of(lows[b], size), size)

        def other(b):
            size = rows >> (b + 1)
            start = lows[b] + (1 - bit_of(b)) * size
            return pl.ds(pl.multiple_of(start, size), size)

        def scatter_copy(c, b):
            size = rows >> (b + 1)
            return remote(
                send1.at[c, other(b), :], recv1.at[b, c, pl.ds(0, size), :], a_ss.at[b], a_rs.at[b, c], {"mp": partner(b)}
            )

        def across_copy(c):
            return remote(
                psum.at[c, seg(low), :], psum.at[c, seg(low), :], x_ss.at[0], x_rs.at[c], {"mp": lax.rem(i + half, n_mp)}
            )

        def gather_copy(c, b):
            return remote(
                psum.at[c, seg(b + 1), :], psum.at[c, seg(b + 1), :], g_ss.at[b], g_rs.at[b, c], {"mp": partner(b)}
            )

        def gather_wait(c, b):
            remote(
                psum.at[c, other(b), :], psum.at[c, other(b), :], g_ss.at[b], g_rs.at[b, c], {"mp": partner(b)}
            ).wait_recv()

        def spread(c):
            if low > 0:
                gather_copy(c, low - 1).start()

        def stage_a(c):
            w1_copies[c].wait()
            term = jnp.dot(base_mp[...], w1_v[c], preferred_element_type=F32)
            if low > 0:
                acc1[c] = term
                send1[c] = term.astype(BF16)
            else:
                psum[c] = term.astype(BF16)

        def stage_b(c):
            for b in range(low):
                scatter_copy(c, b).wait_recv()
                size = rows >> (b + 1)
                term = acc1[c, seg(b + 1), :] + recv1[b, c, 0:size, :].astype(F32)
                if b + 1 < low:
                    acc1[c, seg(b + 1), :] = term
                    send1[c, seg(b + 1), :] = term.astype(BF16)
                    scatter_copy(c, b + 1).start()
                else:
                    psum[c, seg(low), :] = term.astype(BF16)
            across_copy(c).start()
            spread(c)

        def part_copy(c, d):
            return remote(ubuf.at[i, c], ubuf.at[i, c], u_ss.at[d], u_rs.at[i, c], {"mp": lax.rem(i + d, n_mp)})

        def part_wait(c, src):
            remote(ubuf.at[src, c], ubuf.at[src, c], u_ss.at[0], u_rs.at[src, c], {"mp": src}).wait_recv()

        with scope("firstpart"):
            @pl.when(pool_side)
            def _():
                build_onehot()
                pool_m_copy.wait()
                from_pool(base_mp, pool_m, feat)
                stage_a(0)

        with scope("barrier"):
            pl.semaphore_wait(barrier, n_cand - 1 + n_mp - 1)
        for d in range(1, n_cand):
            user_copy(d).start()

        with scope("layer1"):
            @pl.when(pool_side)
            def _():
                if low > 0:
                    scatter_copy(0, 0).start()
                for c in range(1, n1):
                    with scope(f"a{c}"):
                        stage_a(c)
                        if low > 0:
                            scatter_copy(c, 0).start()
                    with scope(f"b{c - 1}"):
                        stage_b(c - 1)
                w2_copy.start()
                with scope(f"b{n1 - 1}"):
                    stage_b(n1 - 1)

            @pl.when(user_side)
            def _():
                with scope("users"):
                    from_all_users()
                with scope("lhs"):
                    rows_of = [user_row(u, i, feat) for u in range(users)]
                    if users == 1:
                        lhs[...] = jnp.broadcast_to(rows_of[0], lhs.shape).astype(BF16)
                    else:
                        place = lax.broadcasted_iota(jnp.int32, lhs.shape, 0)
                        filled = jnp.zeros(lhs.shape, F32)
                        for u in range(users):
                            filled = jnp.where(place == u, rows_of[u], filled)
                        lhs[...] = filled.astype(BF16)
                with scope("um"):
                    for copy in w1_copies:
                        copy.wait()
                    for c in range(n1):
                        term = jnp.dot(lhs[...], w1_v[c], preferred_element_type=F32)
                        ubuf[i, c] = term[0:users]
                        for d in range(n_mp - 1, 0, -1):
                            part_copy(c, d).start()

        with scope("bases"):
            w3_copy.start()

            @pl.when(pool_side)
            def _():
                from_all_users()

            @pl.when(user_side)
            def _():
                from_user(base_mp, i, feat)

                @pl.when(col_pool)
                def _():
                    build_onehot()

                @pl.when(jnp.logical_not(col_pool))
                def _():
                    small_copies[0].wait()

            @pl.when(col_pool)
            def _():
                pool_c_copy.wait()
                from_pool(base_col, pool_c, col)

            @pl.when(jnp.logical_not(col_pool))
            def _():
                from_user(base_col, j, col)

            for copy in small_copies[3:]:
                copy.wait()

        def take_across(c):
            @pl.when(user_side)
            def _():
                with scope(f"across{c}"):
                    across_copy(c).wait_recv()
                spread(c)

        def first_cross(c):
            with scope(f"gw{c}"):
                for b in range(low - 1, -1, -1):
                    gather_wait(c, b)
                    if b > 0:
                        gather_copy(c, b - 1).start()
            with scope(f"pw{c}"):
                @pl.when(user_side)
                def _():
                    for d in range(1, half):
                        part_wait(c, lax.rem(i + d, half))

                @pl.when(pool_side)
                def _():
                    for src in range(half):
                        part_wait(c, src)

            cols = slice(c * cw1, (c + 1) * cw1)
            added = b1_ref[:, cols]
            for src in range(half):
                added = added + ubuf[src, c]
            for p in range(n_mp):
                r = slice(p * block, (p + 1) * block)
                u = user_of(p)
                base = base_col[r, cols].astype(F32)
                cross1[c, r, :] = (base * (psum[c, r, :].astype(F32) + added[u : u + 1]) + base).astype(BF16)

        halves = [slice(g * part, (g + 1) * part) for g in range(2)]
        toward = 1 - 2 * nd

        def z_copy(g, n, way, src, step):
            return remote(
                src.at[n, halves[g], :], zr.at[way, n, halves[g], :], z_ss.at[way], z_rs.at[way, g, n],
                {"cand": j + step},
            )

        def z_wait(g, n, way):
            remote(
                q_send.at[n, halves[g], :], zr.at[way, n, halves[g], :], z_ss.at[way], z_rs.at[way, g, n], {"cand": j}
            ).wait_recv()

        def first_out(n):
            cols = slice(n * cw2, (n + 1) * cw2)
            term = jnp.dot(cross1[n1 - 1], w2_v[(n1 - 1) * cw1 : n1 * cw1, cols], preferred_element_type=F32)
            if n1 > 1:
                term = acc2[:, cols] + term
            owner = (j == i * ratio + (n * cw2) // col).astype(F32)
            inside = (n * cw2) % col
            carried = cross1[inside // cw1, :, inside % cw1 : inside % cw1 + cw2].astype(F32)
            term = base_mp[:, cols].astype(F32) * (term + owner * b2_ref[:, cols]) + owner * carried
            q_send[n] = term.astype(BF16)

        ahead = min(3, n1)
        for c in range(ahead):
            take_across(c)
        for c in range(n1):
            first_cross(c)
            if c + ahead < n1:
                take_across(c + ahead)
            if c == 0:
                w2_copy.wait()
            if c < n1 - 1:
                with scope(f"l2_{c}"):
                    term = jnp.dot(cross1[c], w2_v[c * cw1 : (c + 1) * cw1, :], preferred_element_type=F32)
                    acc2[...] = term if c == 0 else acc2[...] + term
        per = min(2, n2)
        for s in range(0, n2, per):
            with scope(f"q{s}"):
                for n in range(s, min(s + per, n2)):
                    first_out(n)

                @pl.when(end)
                def _():
                    for n in range(s, min(s + per, n2)):
                        z_copy(0, n, nd, q_send, toward).start()

        @pl.when(end)
        def _():
            for n in range(n2):
                z_copy(1, n, nd, q_send, toward).start()

        def near(g, n):
            @pl.when(inner)
            def _():
                with scope(f"near{g}_{n}"):
                    z_wait(g, n, nd)
                zs[nd, n, halves[g], :] = (zr[nd, n, halves[g], :].astype(F32) + q_send[n, halves[g], :].astype(F32)).astype(BF16)
                z_copy(g, n, nd, zs.at[nd], toward).start()

        def far(g, n):
            with scope(f"far{g}_{n}"):
                z_wait(g, n, 1 - nd)

            @pl.when(inner)
            def _():
                zs[1 - nd, n, halves[g], :] = (
                    zr[1 - nd, n, halves[g], :].astype(F32) + q_send[n, halves[g], :].astype(F32)
                ).astype(BF16)
                z_copy(g, n, 1 - nd, zs.at[1 - nd], -toward).start()

        def third(g, n):
            cols = slice(n * cw2, (n + 1) * cw2)
            r = halves[g]
            value = (
                q_send[n, r, :].astype(F32) + zr[0, n, r, :].astype(F32) + zr[1, n, r, :].astype(F32)
            ).astype(BF16)
            x3[r, cols] = value
            if g == 0 and n == 0:
                w3_copy.wait()
            term = jnp.dot(value, w3_v[cols, :], preferred_element_type=F32)
            acc3[r, :] = term if n == 0 else acc3[r, :] + term

        def own_start(d):
            peer = lax.rem(i + d, n_mp)
            return peer, pl.ds(pl.multiple_of(reverse_bits(peer, bits) * block, block), block)

        def last_copy(c, d):
            peer, r = own_start(d)
            cols = slice(c * cw3, (c + 1) * cw3)
            return remote(
                send3.at[r, cols], recv3.at[i, :, cols], c_ss.at[0], c_rs.at[c], {"mp": peer}
            )

        owner3 = (i == j // ratio).astype(F32)

        def epilogue(g):
            r = halves[g]
            same = bit_of(0) == g
            lanes = jnp.zeros((part, 128), F32)
            for c in range(n3):
                cols = slice(c * cw3, (c + 1) * cw3)
                if ratio == 1:
                    carried = x3[r, cols]
                else:
                    carried = x3[r, pl.ds(pl.multiple_of(lax.rem(j, ratio) * col + c * cw3, 128), cw3)]
                term = (
                    base_col[r, cols].astype(F32) * (acc3[r, cols] + owner3 * b3_ref[:, cols])
                    + owner3 * carried.astype(F32)
                )
                acc3[r, cols] = term
                send3[r, cols] = term.astype(BF16)

                @pl.when(same)
                def _():
                    for d in range(2, n_mp, 2):
                        last_copy(c, d).start()

                @pl.when(jnp.logical_not(same))
                def _():
                    for d in range(1, n_mp, 2):
                        last_copy(c, d).start()

            for c in range(n3):
                cols = slice(c * cw3, (c + 1) * cw3)
                scored = acc3[r, cols] * score_ref[cols].astype(F32).reshape(1, cw3)
                for k in range(0, cw3, 128):
                    lanes = lanes + scored[:, k : k + 128]
            q_rows[r, :] = lanes

        events = [(g, n) for g in range(2) for n in range(n2)]
        skew = min(8, n2)
        if max(rows, 128) > rows:
            q_rows[rows:, :] = jnp.zeros((max(rows, 128) - rows, 128), F32)
        for s in range(len(events) + skew):
            if s < len(events):
                near(*events[s])
            if s < skew:
                continue
            g, n = events[s - skew]
            far(g, n)
            with scope(f"third{g}_{n}"):
                third(g, n)
            if n == n2 - 1:
                with scope(f"epi{g}"):
                    epilogue(g)

        with scope("qsend"):
            q_all[me] = jnp.sum(q_rows[...].T, axis=0, keepdims=True)

            def q_copy(d):
                peer = lax.rem(me + d, group)
                return remote(
                    q_all.at[me], q_all.at[me], q_sem.at[0], q_sem.at[1],
                    {"mp": peer // n_cand, "cand": lax.rem(peer, n_cand)},
                )

            def q_start(d, carry):
                q_copy(d).start()
                return carry

            lax.fori_loop(1, group, q_start, 0)

        mine = pl.ds(pl.multiple_of(reverse_bits(i, bits) * block, block), block)
        for c in range(n3):
            cols = slice(c * cw3, (c + 1) * cw3)
            with scope(f"last{c}"):
                came = recv3.at[pl.ds(0, n_mp - 1), :, cols]
                remote(came, came, c_ss.at[0], c_rs.at[c], {"mp": i}).wait_recv()
            term = acc3[mine, cols]
            for d in range(1, n_mp):
                term = term + recv3[lax.rem(i - d + n_mp, n_mp), :, cols].astype(F32)
            out_ref[:, cols] = term.astype(BF16)

        with scope("qwait"):
            rest = q_all.at[pl.ds(0, group - 1)]
            remote(rest, rest, q_sem.at[0], q_sem.at[1], {"cand": j}).wait_recv()
            total = jnp.sum(q_all[...], axis=0)
            for k in range(n_mp):
                p = reverse_bits(k, bits)

                @pl.when(i == k)
                def _():
                    logit_ref[...] = total[:, p * block : (p + 1) * block]

        def sent(ref, sem):
            remote(ref, ref, sem, sem, {"cand": j}).wait_send()

        with scope("sent"):
            sent(others, user_sem.at[0])

            @pl.when(pool_side)
            def _():
                for b in range(low):
                    sent(recv1.at[b, :, pl.ds(0, rows >> (b + 1)), :], a_ss.at[b])
                sent(psum.at[:, seg(low), :], x_ss.at[0])

            @pl.when(user_side)
            def _():
                for d in range(1, n_mp):
                    sent(ubuf.at[i], u_ss.at[d])

            for b in range(low):
                sent(psum.at[:, seg(b + 1), :], g_ss.at[b])
            sent(q_send, z_ss.at[nd])

            @pl.when(inner)
            def _():
                sent(q_send, z_ss.at[1 - nd])

            sent(recv3.at[pl.ds(0, n_mp - 1)], c_ss.at[0])
            sent(rest, q_sem.at[0])

    return kernel


def solution(mesh):
    n_mp, n_cand = mesh.shape["mp"], mesh.shape["cand"]

    def body(
        user_feats, user_slot, cand_pool, cand_ids, first_weight, first_bias,
        second_weight, second_bias, third_weight, third_bias, score_weight,
    ):
        slots_each, half_width = user_feats.shape
        users, per_user = cand_ids.shape
        rows = users * per_user
        pool_count = cand_pool.shape[0]
        feat, col = first_weight.shape
        n1 = max(1, col // 512)
        n2 = max(1, feat // 256)
        n3 = max(1, col // 512)
        lhs_rows = -(-users // 16) * 16
        cw1, cw2 = col // n1, feat // n2
        bits = n_mp.bit_length() - 1
        low = max(1, bits - 1)
        half = n_mp // 2
        block = rows // n_mp
        group = n_mp * n_cand
        shapes = (rows, per_user, users, slots_each, half_width, pool_count, feat, col, n1, n2, n3, lhs_rows)
        vmem = pl.BlockSpec(memory_space=pltpu.VMEM)
        hbm = pl.BlockSpec(memory_space=pl.ANY)
        dma = pltpu.SemaphoreType.DMA
        crossed, logits = pl.pallas_call(
            make_kernel(n_mp, n_cand, shapes),
            out_shape=(
                pltpu.VMEM((block, col), BF16),
                pltpu.VMEM((1, block), F32),
            ),
            in_specs=[hbm] * 11,
            out_specs=(vmem, vmem),
            scratch_shapes=[
                pltpu.SMEM((1, users), jnp.int32),
                pltpu.VMEM((users, per_user), jnp.int32),
                pltpu.VMEM((1, col), F32),
                pltpu.VMEM((1, feat), F32),
                pltpu.VMEM((1, col), F32),
                pltpu.VMEM((col,), BF16),
                dma((7,)),
                pltpu.VMEM((n_cand, slots_each, half_width), BF16),
                pltpu.VMEM((pool_count, feat), BF16),
                pltpu.VMEM((pool_count, col), BF16),
                pltpu.VMEM((n1, feat, cw1), BF16),
                pltpu.VMEM((col, feat), BF16),
                pltpu.VMEM((feat, col), BF16),
                pltpu.VMEM((rows, pool_count), BF16),
                pltpu.VMEM((rows, feat), BF16),
                pltpu.VMEM((rows, col), BF16),
                pltpu.VMEM((lhs_rows, feat), BF16),
                pltpu.VMEM((n1, rows, cw1), F32),
                pltpu.VMEM((n1, rows, cw1), BF16),
                pltpu.VMEM((low, n1, rows // 2, cw1), BF16),
                pltpu.VMEM((n1, rows, cw1), BF16),
                pltpu.VMEM((half, n1, users, cw1), F32),
                pltpu.VMEM((n1, rows, cw1), BF16),
                pltpu.VMEM((rows, feat), F32),
                pltpu.VMEM((n2, rows, cw2), BF16),
                pltpu.VMEM((2, n2, rows, cw2), BF16),
                pltpu.VMEM((2, n2, rows, cw2), BF16),
                pltpu.VMEM((rows, feat), BF16),
                pltpu.VMEM((rows, col), F32),
                pltpu.VMEM((rows, col), BF16),
                pltpu.VMEM((n_mp, block, col), BF16),
                pltpu.VMEM((max(rows, 128), 128), F32),
                pltpu.VMEM((group, 1, max(rows, 128)), F32),
                dma((4 + n1,)),
                dma((2,)),
                dma((low,)),
                dma((low, n1)),
                dma((1,)),
                dma((n1,)),
                dma((low,)),
                dma((low, n1)),
                dma((n_mp,)),
                dma((half, n1)),
                dma((2,)),
                dma((2, 2, n2)),
                dma((1,)),
                dma((n3,)),
                dma((2,)),
            ],
            compiler_params=pltpu.CompilerParams(
                collective_id=0, has_side_effects=True, vmem_limit_bytes=67043328 - 3000 * 1024
            ),
        )(
            user_feats, user_slot.reshape(1, -1), cand_pool, cand_ids, first_weight, first_bias.reshape(1, -1),
            second_weight, second_bias.reshape(1, -1), third_weight, third_bias.reshape(1, -1),
            score_weight,
        )
        crossed, logits = pl.pallas_call(
            hand_on,
            out_shape=(
                jax.ShapeDtypeStruct((block, col), BF16),
                jax.ShapeDtypeStruct((1, block), F32),
            ),
            in_specs=[vmem, vmem],
            out_specs=(hbm, hbm),
            scratch_shapes=[dma((2,))],
            compiler_params=pltpu.CompilerParams(vmem_limit_bytes=1024 * 1024),
        )(crossed, logits)
        return crossed, logits.reshape(-1)

    in_specs = (
        P(("groups", "cand"), None),
        P("groups"),
        P("groups", None),
        P("groups", None),
        P("mp", "cand"),
        P("cand"),
        P("cand", "mp"),
        P("mp"),
        P("mp", "cand"),
        P("cand"),
        P("cand"),
    )
    out_specs = (P(("groups", "mp"), "cand"), P(("groups", "mp")))
    return jax.shard_map(body, mesh=mesh, in_specs=in_specs, out_specs=out_specs, check_vma=False)
```

```python
import contextlib

import jax
import jax.numpy as jnp
from jax import lax
from jax.experimental import pallas as pl
from jax.experimental.pallas import tpu as pltpu
from jax.sharding import PartitionSpec as P

MESH = pl.DeviceIdType.MESH
F32 = jnp.float32
BF16 = jnp.bfloat16


def scope(name):
    return contextlib.nullcontext()


def hand_on(crossed_ref, logit_ref, crossed_hbm, logit_hbm, sem):
    copies = [
        pltpu.make_async_copy(crossed_ref, crossed_hbm, sem.at[0]),
        pltpu.make_async_copy(logit_ref, logit_hbm, sem.at[1]),
    ]
    for copy in copies:
        copy.start()
    for copy in copies:
        copy.wait()


def make_kernel(n_mp, n_cand, shapes):
    rows, per_user, users, slots_each, half_width, pool_count, feat, col, cuts, ucuts, zcuts, n3 = shapes
    cw3 = col // n3
    n1 = len(cuts)
    bits = n_mp.bit_length() - 1
    low = bits - 1
    half = n_mp // 2
    block = rows // n_mp
    ratio = feat // col
    group = n_mp * n_cand
    part = rows // 2
    q_width = max(part, 128)
    first_pool_col = half_width // col

    def user_of(p):
        return (p * block) // per_user

    def kernel(
        user_hbm, slot_hbm, pool_hbm, ids_hbm, w1_hbm, b1_hbm, w2_hbm, b2_hbm, w3_hbm, b3_hbm, score_hbm,
        out_ref, logit_ref,
        slot_ref, ids_ref, b1_ref, b2_ref, b3_ref, score_ref, small_sem, slots, ucol, pool_m, pool_c, w1_v, w2_v, w3_v,
        onehot, base_mp, base_col, lhs, acc1, send1, recv1, psum, ubuf, cross1, acc2, q_send, zr, zs, x3, acc3, send3, recv3,
        q_rows, q_mine, q_all,
        w_sem, user_sem, ucol_sem, ready, a_ss, a_rs, x_ss, x_rs, g_ss, g_rs, u_ss, u_rs, z_ss, z_rs, c_ss, c_rs, q_sem,
    ):
        i = lax.axis_index("mp")
        j = lax.axis_index("cand")
        me = i * n_cand + j
        user_side = i < half
        pool_side = jnp.logical_not(user_side)

        def remote(src, dst, ss, rs, where):
            return pltpu.make_async_remote_copy(
                src_ref=src, dst_ref=dst, send_sem=ss, recv_sem=rs, device_id=where, device_id_type=MESH
            )

        barrier = pltpu.get_barrier_semaphore()
        with scope("greet"):
            def greet(d, carry):
                pl.semaphore_signal(barrier, inc=1, device_id={"cand": lax.rem(j + d, n_cand)}, device_id_type=MESH)
                return carry

            @pl.when(user_side)
            def _():
                lax.fori_loop(1, n_cand, greet, 0, unroll=n_cand <= 4)
                for d in range(1, n_mp):
                    pl.semaphore_signal(barrier, inc=1, device_id={"mp": lax.rem(i + d, n_mp)}, device_id_type=MESH)

            @pl.when(pool_side)
            def _():
                for d in range(1, half):
                    pl.semaphore_signal(
                        barrier, inc=1, device_id={"mp": half + lax.rem(i + d, half)}, device_id_type=MESH
                    )

                @pl.when(j > 0)
                def _():
                    pl.semaphore_signal(barrier, inc=1, device_id={"cand": j - 1}, device_id_type=MESH)

                @pl.when(j < n_cand - 1)
                def _():
                    pl.semaphore_signal(barrier, inc=1, device_id={"cand": j + 1}, device_id_type=MESH)

        small_copies = [
            pltpu.make_async_copy(src, dst, small_sem.at[k])
            for k, (src, dst) in enumerate(
                (
                    (ids_hbm, ids_ref), (slot_hbm, slot_ref), (user_hbm, slots.at[j]), (b1_hbm, b1_ref),
                    (b2_hbm, b2_ref), (b3_hbm, b3_ref), (score_hbm, score_ref),
                )
            )
        ]
        m_start = pl.multiple_of(jnp.maximum(i - half, 0) * feat, 128)
        c_start = pl.multiple_of(jnp.maximum(j - first_pool_col, 0) * col, 128)
        pool_m_copy = pltpu.make_async_copy(pool_hbm.at[:, pl.ds(m_start, feat)], pool_m, w_sem.at[0])
        pool_c_copy = pltpu.make_async_copy(pool_hbm.at[:, pl.ds(c_start, col)], pool_c, w_sem.at[1])
        w1_copies = [
            pltpu.make_async_copy(w1_hbm.at[:, cut], w1_v.at[:, cut], w_sem.at[2 + c]) for c, cut in enumerate(cuts)
        ]
        w2_copy = pltpu.make_async_copy(w2_hbm, w2_v, w_sem.at[2 + n1])
        w3_copy = pltpu.make_async_copy(w3_hbm, w3_v, w_sem.at[3 + n1])
        col_pool = j >= first_pool_col
        with scope("loads"):
            for copy in small_copies[:3]:
                copy.start()

            @pl.when(pool_side)
            def _():
                pool_m_copy.start()

            for copy in w1_copies:
                copy.start()
            for copy in small_copies[3:]:
                copy.start()

            @pl.when(col_pool)
            def _():
                pool_c_copy.start()

            @pl.when(user_side)
            def _():
                w2_copy.start()

            end = jnp.logical_or(j == 0, j == n_cand - 1)
            inner = jnp.logical_not(end)
            nd = (j >= (n_cand + 1) // 2).astype(jnp.int32)

            @pl.when(end)
            def _():
                zr[nd] = jnp.zeros(zr.shape[1:], BF16)

        def build_onehot():
            with scope("onehot"):
                small_copies[0].wait()
                for u in range(users):
                    hot = (
                        lax.broadcasted_iota(jnp.int32, (pool_count, per_user), 0) == ids_ref[u : u + 1, :]
                    ).astype(F32).T
                    for p in range(n_mp):
                        first = p * block
                        if first // per_user == u:
                            off = first % per_user
                            onehot[p * block : (p + 1) * block, :] = hot[off : off + block].astype(BF16)

        def from_pool(dst, src, width):
            for c in range(0, width, 256):
                dst[:, c : c + 256] = jnp.dot(onehot[...], src[:, c : c + 256], preferred_element_type=F32).astype(BF16)

        def user_row(u, index, width):
            start = pl.multiple_of(index * width, 128)
            slot = slot_ref[0, u]
            row = slots[slot // slots_each, :, pl.ds(start, width)].astype(F32)
            if slots_each > 1:
                pick = lax.broadcasted_iota(jnp.int32, row.shape, 0) == lax.rem(slot, slots_each)
                row = jnp.sum(jnp.where(pick, row, 0.0), axis=0, keepdims=True)
            return row

        def from_user(dst, index, width):
            rows_of = [user_row(u, index, width) for u in range(users)]
            for p in range(n_mp):
                dst[p * block : (p + 1) * block, :] = jnp.broadcast_to(rows_of[user_of(p)], (block, width)).astype(BF16)

        def user_copy(k):
            d = jnp.where(j < n_cand // 2, n_cand - k, k)
            return remote(user_hbm, slots.at[j], user_sem.at[0], user_sem.at[1], {"cand": lax.rem(j + d, n_cand)})

        def ucol_copy():
            return remote(ucol, ucol, ucol_sem.at[0], ucol_sem.at[1], {"mp": lax.rem(i + half, n_mp)})

        others = slots.at[pl.ds(0, n_cand - 1)]

        def from_all_users():
            remote(others, others, user_sem.at[0], user_sem.at[1], {"cand": j}).wait_recv()
            small_copies[1].wait()

        def bit_of(b):
            return lax.rem(i // (1 << b), 2)

        def partner(b):
            return i + (1 << b) * (1 - 2 * bit_of(b))

        lows = [0]
        for b in range(bits):
            lows.append(lows[b] + bit_of(b) * (rows >> (b + 1)))

        def seg(b):
            size = rows >> b
            if b == 0:
                return pl.ds(0, rows)
            return pl.ds(pl.multiple_of(lows[b], size), size)

        def other(b):
            size = rows >> (b + 1)
            start = lows[b] + (1 - bit_of(b)) * size
            return pl.ds(pl.multiple_of(start, size), size)

        def scatter_copy(c, b):
            size = rows >> (b + 1)
            return remote(
                send1.at[other(b), cuts[c]], recv1.at[b, pl.ds(0, size), cuts[c]], a_ss.at[b], a_rs.at[b, c], {"mp": partner(b)}
            )

        def across_copy(c):
            return remote(
                psum.at[seg(low), cuts[c]], psum.at[seg(low), cuts[c]], x_ss.at[0], x_rs.at[c], {"mp": lax.rem(i + half, n_mp)}
            )

        def gather_copy(c, b):
            return remote(
                psum.at[seg(b + 1), cuts[c]], psum.at[seg(b + 1), cuts[c]], g_ss.at[b], g_rs.at[b, c], {"mp": partner(b)}
            )

        def gather_wait(c, b):
            remote(
                psum.at[other(b), cuts[c]], psum.at[other(b), cuts[c]], g_ss.at[b], g_rs.at[b, c], {"mp": partner(b)}
            ).wait_recv()

        def spread(c):
            if low > 0:
                gather_copy(c, low - 1).start()

        def stage_a(c):
            w1_copies[c].wait()
            term = jnp.dot(base_mp[...], w1_v[:, cuts[c]], preferred_element_type=F32)
            if low > 0:
                acc1[:, cuts[c]] = term
                send1[:, cuts[c]] = term.astype(BF16)
            else:
                psum[:, cuts[c]] = term.astype(BF16)

        def stage_b(c):
            for b in range(low):
                scatter_copy(c, b).wait_recv()
                size = rows >> (b + 1)
                term = acc1[seg(b + 1), cuts[c]] + recv1[b, 0:size, cuts[c]].astype(F32)
                if b + 1 < low:
                    acc1[seg(b + 1), cuts[c]] = term
                    send1[seg(b + 1), cuts[c]] = term.astype(BF16)
                    scatter_copy(c, b + 1).start()
                else:
                    psum[seg(low), cuts[c]] = term.astype(BF16)
            across_copy(c).start()
            spread(c)

        def part_copy(c, d):
            return remote(ubuf.at[i, :, ucuts[c]], ubuf.at[i, :, ucuts[c]], u_ss.at[0], u_rs.at[c], {"mp": lax.rem(i + d, n_mp)})

        def part_wait(c, count):
            came = ubuf.at[pl.ds(0, count), :, ucuts[c]]
            remote(came, came, u_ss.at[0], u_rs.at[c], {"cand": j}).wait_recv()

        with scope("firstpart"):
            @pl.when(pool_side)
            def _():
                build_onehot()
                pool_m_copy.wait()
                from_pool(base_mp, pool_m, feat)

        neighbours = (j > 0).astype(jnp.int32) + (j < n_cand - 1).astype(jnp.int32)
        with scope("barrier"):
            pl.semaphore_wait(barrier, jnp.where(user_side, n_cand - 1 + half - 1, neighbours + n_mp - 1))

        with scope("layer1"):
            @pl.when(pool_side)
            def _():
                for d in range(half):
                    pl.semaphore_signal(ready.at[0], inc=1, device_id={"mp": d}, device_id_type=MESH)
                for c in range(n1 + 2):
                    if c < n1:
                        with scope(f"a{c}"):
                            stage_a(c)
                            if low > 0:
                                scatter_copy(c, 0).start()
                        if c == n1 - 1:
                            w2_copy.start()
                    if c >= 2:
                        with scope(f"b{c - 2}"):
                            stage_b(c - 2)

            @pl.when(user_side)
            def _():
                for k in range(1, n_cand):
                    user_copy(k).start()
                with scope("early"):
                    @pl.when(col_pool)
                    def _():
                        build_onehot()
                        pool_c_copy.wait()
                        from_pool(base_col, pool_c, col)

                    @pl.when(jnp.logical_not(col_pool))
                    def _():
                        small_copies[0].wait()

                    for copy in w1_copies:
                        copy.wait()
                    small_copies[2].wait()
                    pl.semaphore_wait(ready.at[0], half)
                with scope("users"):
                    from_all_users()
                rows_of = [user_row(u, i, feat) for u in range(users)]
                if users == 1:
                    lhs[...] = jnp.broadcast_to(rows_of[0], lhs.shape).astype(BF16)
                else:
                    place = lax.broadcasted_iota(jnp.int32, lhs.shape, 0)
                    filled = jnp.zeros(lhs.shape, F32)
                    for u in range(users):
                        filled = jnp.where(place == u, rows_of[u], filled)
                    lhs[...] = filled.astype(BF16)
                for c, cut in enumerate(ucuts):
                    with scope(f"um{c}"):
                        term = jnp.dot(lhs[...], w1_v[:, cut], preferred_element_type=F32)
                        ubuf[i, :, cut] = term[0:users]
                        for d in range(n_mp - 1, 0, -1):
                            part_copy(c, d).start()
                    if c == 0:
                        @pl.when(jnp.logical_not(col_pool))
                        def _():
                            for u in range(users):
                                ucol[u : u + 1, :] = user_row(u, j, col).astype(BF16)
                            ucol_copy().start()

        def take_across(c):
            @pl.when(user_side)
            def _():
                with scope(f"across{c}"):
                    across_copy(c).wait_recv()
                spread(c)

        ahead = min(2, n1)
        with scope("bases"):
            w3_copy.start()

            for c in range(ahead):
                take_across(c)

            @pl.when(user_side)
            def _():
                from_user(base_mp, i, feat)

            @pl.when(jnp.logical_and(col_pool, pool_side))
            def _():
                pool_c_copy.wait()
                from_pool(base_col, pool_c, col)

            @pl.when(jnp.logical_not(col_pool))
            def _():
                @pl.when(pool_side)
                def _():
                    ucol_copy().wait_recv()

                for p in range(n_mp):
                    u = user_of(p)
                    value = ucol[u : u + 1, :].astype(F32)
                    base_col[p * block : (p + 1) * block, :] = jnp.broadcast_to(value, (block, col)).astype(BF16)

            for copy in small_copies[3:]:
                copy.wait()

            @pl.when(pool_side)
            def _():
                for copy in small_copies[1:3]:
                    copy.wait()

        def first_cross(c):
            with scope(f"gw{c}"):
                for b in range(low - 1, -1, -1):
                    gather_wait(c, b)
                    if b > 0:
                        gather_copy(c, b - 1).start()
            for u, ucut in enumerate(ucuts):
                if ucut.start != cuts[c].start:
                    continue
                with scope(f"pw{u}"):
                    @pl.when(user_side)
                    def _():
                        if half > 1:
                            part_wait(u, half - 1)

                    @pl.when(pool_side)
                    def _():
                        part_wait(u, half)

            cols = cuts[c]
            added = b1_ref[:, cols]
            for src in range(half):
                added = added + ubuf[src, :, cols]
            for p in range(n_mp):
                r = slice(p * block, (p + 1) * block)
                u = user_of(p)
                base = base_col[r, cols].astype(F32)
                cross1[r, cols] = (base * (psum[r, cols].astype(F32) + added[u : u + 1]) + base).astype(BF16)

        halves = [slice(g * part, (g + 1) * part) for g in range(2)]
        toward = 1 - 2 * nd

        def z_copy(g, n, way, src, step):
            at = (halves[g], zcuts[g][n])
            return remote(
                src.at[at], zr.at[(way,) + at], z_ss.at[way], z_rs.at[way, g, n], {"cand": j + step}
            )

        def z_wait(g, n, way):
            at = (halves[g], zcuts[g][n])
            remote(q_send.at[at], zr.at[(way,) + at], z_ss.at[way], z_rs.at[way, g, n], {"cand": j}).wait_recv()

        def first_out(cols):
            last = cuts[n1 - 1]
            term = jnp.dot(cross1[:, last], w2_v[last, cols], preferred_element_type=F32)
            if n1 > 1:
                term = acc2[:, cols] + term
            owner = (j == i * ratio + cols.start // col).astype(F32)
            inside = cols.start % col
            carried = cross1[:, inside : inside + cols.stop - cols.start].astype(F32)
            term = base_mp[:, cols].astype(F32) * (term + owner * b2_ref[:, cols]) + owner * carried
            q_send[:, cols] = term.astype(BF16)

        for c in range(n1):
            first_cross(c)
            if c + ahead < n1:
                take_across(c + ahead)
            if c == 0:
                w2_copy.wait()
            if c < n1 - 1:
                with scope(f"l2_{c}"):
                    term = jnp.dot(cross1[:, cuts[c]], w2_v[cuts[c], :], preferred_element_type=F32)
                    acc2[...] = term if c == 0 else acc2[...] + term
        for s in range(0, len(zcuts[0]), 2):
            with scope(f"q{s}"):
                for cols in zcuts[0][s : s + 2]:
                    first_out(cols)

                @pl.when(end)
                def _():
                    for n in range(s, min(s + 2, len(zcuts[0]))):
                        z_copy(0, n, nd, q_send, toward).start()

        @pl.when(end)
        def _():
            for g in range(1, len(zcuts)):
                for n in range(len(zcuts[g])):
                    z_copy(g, n, nd, q_send, toward).start()

        def pass_on(g, n, way, step):
            at = (halves[g], zcuts[g][n])
            zs[(way,) + at] = (zr[(way,) + at].astype(F32) + q_send[at].astype(F32)).astype(BF16)
            z_copy(g, n, way, zs.at[way], step).start()

        def near(g, n):
            @pl.when(inner)
            def _():
                with scope(f"near{g}_{n}"):
                    z_wait(g, n, nd)
                pass_on(g, n, nd, toward)

        def far(g, n):
            with scope(f"far{g}_{n}"):
                z_wait(g, n, 1 - nd)

            @pl.when(inner)
            def _():
                pass_on(g, n, 1 - nd, -toward)

        def third(g, n):
            cols = zcuts[g][n]
            r = halves[g]
            value = (
                q_send[r, cols].astype(F32) + zr[0, r, cols].astype(F32) + zr[1, r, cols].astype(F32)
            ).astype(BF16)
            x3[r, cols] = value
            if g == 0 and n == 0:
                w3_copy.wait()
            term = jnp.dot(value, w3_v[cols, :], preferred_element_type=F32)
            acc3[r, :] = term if n == 0 else acc3[r, :] + term

        side = i // half

        def last_copy(c, peer):
            r = pl.ds(pl.multiple_of(peer * block, block), block)
            cols = slice(c * cw3, (c + 1) * cw3)
            return remote(send3.at[r, cols], recv3.at[i, :, cols], c_ss.at[0], c_rs.at[c], {"mp": peer})

        owner3 = (i == j // ratio).astype(F32)

        def q_copy(g, di, dj):
            return remote(
                q_mine.at[g], q_all.at[me], q_sem.at[0], q_sem.at[1],
                {"mp": g * half + lax.rem(i + di, half), "cand": lax.rem(j + dj, n_cand)},
            )

        def send_scores(g):
            q_mine[g] = jnp.sum(q_rows[...].T, axis=0, keepdims=True)
            same = side == g

            @pl.when(same)
            def _():
                q_all[me] = q_mine[g]

            def each(dj, carry):
                for di in range(half):
                    q_copy(g, di, dj).start()
                return carry

            far_first = [n_cand // 2] + [d for k in range(1, (n_cand + 1) // 2) for d in (n_cand // 2 - k, n_cand // 2 + k)]
            if n_cand <= 4:
                for dj in far_first:
                    if dj:
                        each(dj, 0)
            else:
                lax.fori_loop(1, n_cand, each, 0)
            for di in range(1, half):
                q_copy(g, di, 0).start()

            @pl.when(jnp.logical_not(same))
            def _():
                q_copy(g, 0, 0).start()

        def epilogue(g):
            r = halves[g]
            same = side == g
            for c in range(n3):
                cols = slice(c * cw3, (c + 1) * cw3)
                if ratio == 1:
                    carried = x3[r, cols]
                else:
                    carried = x3[r, pl.ds(pl.multiple_of(lax.rem(j, ratio) * col + c * cw3, 128), cw3)]
                term = (
                    base_col[r, cols].astype(F32) * (acc3[r, cols] + owner3 * b3_ref[:, cols])
                    + owner3 * carried.astype(F32)
                )
                acc3[r, cols] = term
                send3[r, cols] = term.astype(BF16)

                for d in range(1, half):
                    last_copy(c, g * half + lax.rem(i + d, half)).start()

                @pl.when(jnp.logical_not(same))
                def _():
                    last_copy(c, g * half + lax.rem(i, half)).start()

            lanes = jnp.zeros((part, 128), F32)
            for k in range(0, col, 128):
                lanes = lanes + acc3[r, k : k + 128] * score_ref[k : k + 128].astype(F32).reshape(1, 128)
            q_rows[0:part, :] = lanes
            send_scores(g)

        events = [(g, n) for g in range(2) for n in range(len(zcuts[g]))]
        if q_width > part:
            q_rows[part:, :] = jnp.zeros((q_width - part, 128), F32)

        def stream(skew):
            first_done = max(len(zcuts[0]) - 1, len(events) - skew)
            for s in range(len(events) + skew):
                if s < len(events):
                    near(*events[s])
                if s < skew:
                    continue
                g, n = events[s - skew]
                far(g, n)
                with scope(f"third{g}_{n}"):
                    third(g, n)
                if s - skew == first_done:
                    with scope("epi0"):
                        epilogue(0)
            with scope("epi1"):
                epilogue(1)

        @pl.when(nd == 0)
        def _():
            stream(min(13, len(events)))

        @pl.when(nd == 1)
        def _():
            stream(min(5, len(events)))

        mine = pl.ds(pl.multiple_of(i * block, block), block)
        for c in range(n3):
            cols = slice(c * cw3, (c + 1) * cw3)
            with scope(f"last{c}"):
                came = recv3.at[pl.ds(0, n_mp - 1), :, cols]
                remote(came, came, c_ss.at[0], c_rs.at[c], {"mp": i}).wait_recv()
            term = acc3[mine, cols]
            for d in range(1, n_mp):
                term = term + recv3[lax.rem(i - d + n_mp, n_mp), :, cols].astype(F32)
            out_ref[:, cols] = term.astype(BF16)

        with scope("qwait"):
            rest = q_all.at[pl.ds(0, group - 1)]
            remote(rest, rest, q_sem.at[0], q_sem.at[1], {"cand": j}).wait_recv()
            total = jnp.sum(q_all[...], axis=0)
            for k in range(n_mp):
                p = k % half

                @pl.when(i == k)
                def _():
                    logit_ref[...] = total[:, p * block : (p + 1) * block]

        def sent(ref, sem):
            remote(ref, ref, sem, sem, {"cand": j}).wait_send()

        with scope("sent"):
            @pl.when(pool_side)
            def _():
                for b in range(low):
                    sent(recv1.at[b, pl.ds(0, rows >> (b + 1)), :], a_ss.at[b])
                sent(psum.at[seg(low), :], x_ss.at[0])

            @pl.when(user_side)
            def _():
                sent(others, user_sem.at[0])

                @pl.when(jnp.logical_not(col_pool))
                def _():
                    sent(ucol, ucol_sem.at[0])

                sent(ubuf.at[pl.ds(0, n_mp - 1)], u_ss.at[0])

            for b in range(low):
                sent(psum.at[seg(b + 1), :], g_ss.at[b])
            sent(q_send, z_ss.at[nd])

            @pl.when(inner)
            def _():
                sent(q_send, z_ss.at[1 - nd])

            sent(recv3.at[pl.ds(0, n_mp - 1)], c_ss.at[0])
            sent(rest, q_sem.at[0])

    return kernel


def solution(mesh):
    n_mp, n_cand = mesh.shape["mp"], mesh.shape["cand"]

    def body(
        user_feats, user_slot, cand_pool, cand_ids, first_weight, first_bias,
        second_weight, second_bias, third_weight, third_bias, score_weight,
    ):
        slots_each, half_width = user_feats.shape
        users, per_user = cand_ids.shape
        rows = users * per_user
        pool_count = cand_pool.shape[0]
        feat, col = first_weight.shape
        wide = min(512, col)
        ucuts = [slice(k, k + wide) for k in range(0, col, wide)]
        cuts = list(ucuts)
        step = min(256, col, feat)
        zcuts = [[slice(k, k + step) for k in range(0, feat, step)] for _ in range(2)]
        if step > 128:
            zcuts[1][-1:] = [slice(feat - step, feat - step // 2), slice(feat - step // 2, feat)]
        n1, n2 = len(cuts), len(zcuts[1])
        n3 = max(1, col // 512)
        lhs_rows = -(-users // 16) * 16
        bits = n_mp.bit_length() - 1
        low = max(1, bits - 1)
        half = n_mp // 2
        block = rows // n_mp
        group = n_mp * n_cand
        shapes = (rows, per_user, users, slots_each, half_width, pool_count, feat, col, cuts, ucuts, zcuts, n3)
        vmem = pl.BlockSpec(memory_space=pltpu.VMEM)
        hbm = pl.BlockSpec(memory_space=pl.ANY)
        dma = pltpu.SemaphoreType.DMA
        crossed, logits = pl.pallas_call(
            make_kernel(n_mp, n_cand, shapes),
            out_shape=(
                pltpu.VMEM((block, col), BF16),
                pltpu.VMEM((1, block), F32),
            ),
            in_specs=[hbm] * 11,
            out_specs=(vmem, vmem),
            scratch_shapes=[
                pltpu.SMEM((1, users), jnp.int32),
                pltpu.VMEM((users, per_user), jnp.int32),
                pltpu.VMEM((1, col), F32),
                pltpu.VMEM((1, feat), F32),
                pltpu.VMEM((1, col), F32),
                pltpu.VMEM((col,), BF16),
                dma((7,)),
                pltpu.VMEM((n_cand, slots_each, half_width), BF16),
                pltpu.VMEM((users, col), BF16),
                pltpu.VMEM((pool_count, feat), BF16),
                pltpu.VMEM((pool_count, col), BF16),
                pltpu.VMEM((feat, col), BF16),
                pltpu.VMEM((col, feat), BF16),
                pltpu.VMEM((feat, col), BF16),
                pltpu.VMEM((rows, pool_count), BF16),
                pltpu.VMEM((rows, feat), BF16),
                pltpu.VMEM((rows, col), BF16),
                pltpu.VMEM((lhs_rows, feat), BF16),
                pltpu.VMEM((rows, col), F32),
                pltpu.VMEM((rows, col), BF16),
                pltpu.VMEM((low, rows // 2, col), BF16),
                pltpu.VMEM((rows, col), BF16),
                pltpu.VMEM((n_mp, users, col), F32),
                pltpu.VMEM((rows, col), BF16),
                pltpu.VMEM((rows, feat), F32),
                pltpu.VMEM((rows, feat), BF16),
                pltpu.VMEM((2, rows, feat), BF16),
                pltpu.VMEM((2, rows, feat), BF16),
                pltpu.VMEM((rows, feat), BF16),
                pltpu.VMEM((rows, col), F32),
                pltpu.VMEM((rows, col), BF16),
                pltpu.VMEM((n_mp, block, col), BF16),
                pltpu.VMEM((max(rows // 2, 128), 128), F32),
                pltpu.VMEM((2, 1, max(rows // 2, 128)), F32),
                pltpu.VMEM((group, 1, max(rows // 2, 128)), F32),
                dma((4 + n1,)),
                dma((2,)),
                dma((2,)),
                pltpu.SemaphoreType.REGULAR((1,)),
                dma((low,)),
                dma((low, n1)),
                dma((1,)),
                dma((n1,)),
                dma((low,)),
                dma((low, n1)),
                dma((1,)),
                dma((len(ucuts),)),
                dma((2,)),
                dma((2, 2, n2)),
                dma((1,)),
                dma((n3,)),
                dma((2,)),
            ],
            compiler_params=pltpu.CompilerParams(
                collective_id=0, has_side_effects=True, vmem_limit_bytes=67043328 - 3000 * 1024
            ),
        )(
            user_feats, user_slot.reshape(1, -1), cand_pool, cand_ids, first_weight, first_bias.reshape(1, -1),
            second_weight, second_bias.reshape(1, -1), third_weight, third_bias.reshape(1, -1),
            score_weight,
        )
        crossed, logits = pl.pallas_call(
            hand_on,
            out_shape=(
                jax.ShapeDtypeStruct((block, col), BF16),
                jax.ShapeDtypeStruct((1, block), F32),
            ),
            in_specs=[vmem, vmem],
            out_specs=(hbm, hbm),
            scratch_shapes=[dma((2,))],
            compiler_params=pltpu.CompilerParams(vmem_limit_bytes=1024 * 1024),
        )(crossed, logits)
        return crossed, logits.reshape(-1)

    in_specs = (
        P(("groups", "cand"), None),
        P("groups"),
        P("groups", None),
        P("groups", None),
        P("mp", "cand"),
        P("cand"),
        P("cand", "mp"),
        P("mp"),
        P("mp", "cand"),
        P("cand"),
        P("cand"),
    )
    out_specs = (P(("groups", "mp"), "cand"), P(("groups", "mp")))
    return jax.shard_map(body, mesh=mesh, in_specs=in_specs, out_specs=out_specs, check_vma=False)
```

```python
import contextlib

import jax
import jax.numpy as jnp
from jax import lax
from jax.experimental import pallas as pl
from jax.experimental.pallas import tpu as pltpu
from jax.sharding import PartitionSpec as P

MESH = pl.DeviceIdType.MESH
F32 = jnp.float32
BF16 = jnp.bfloat16


def scope(name):
    return contextlib.nullcontext()


def hand_on(crossed_ref, logit_ref, crossed_hbm, logit_hbm, sem):
    copies = [
        pltpu.make_async_copy(crossed_ref, crossed_hbm, sem.at[0]),
        pltpu.make_async_copy(logit_ref, logit_hbm, sem.at[1]),
    ]
    for copy in copies:
        copy.start()
    for copy in copies:
        copy.wait()


def make_kernel(n_mp, n_cand, shapes):
    rows, per_user, users, slots_each, half_width, pool_count, feat, col, cuts, ucuts, zcuts, spans, n3 = shapes
    cw3 = col // n3
    n1 = len(cuts)
    bits = n_mp.bit_length() - 1
    low = bits - 1
    half = n_mp // 2
    block = rows // n_mp
    ratio = feat // col
    group = n_mp * n_cand
    halves = [slice(lo * block, hi * block) for lo, hi in spans]
    events = [(g, n) for g in range(len(spans)) for n in range(len(zcuts[g]))]
    place = {event: k for k, event in enumerate(events)}
    q_width = max([128] + [r.stop - r.start for r in halves])
    first_pool_col = half_width // col

    def user_of(p):
        return (p * block) // per_user

    def kernel(
        user_hbm, slot_hbm, pool_hbm, ids_hbm, w1_hbm, b1_hbm, w2_hbm, b2_hbm, w3_hbm, b3_hbm, score_hbm,
        out_ref, logit_ref,
        slot_ref, ids_ref, b1_ref, b2_ref, b3_ref, score_ref, small_sem, slots, urow, ucol, pool_m, pool_c, w1_v, w2_v, w3_v,
        onehot, base_mp, base_col, lhs, acc1, send1, recv1, psum, ubuf, cross1, acc2, q_send, zr, zs, ze, zf, qe, x3, acc3, send3, recv3,
        q_rows, q_mine, q_all,
        w_sem, user_sem, urow_ss, urow_rs, ucol_sem, ready, a_ss, a_rs, x_ss, x_rs, g_ss, g_rs, u_ss, u_rs, z_ss, z_rs, ze_rs, qe_ss, qe_rs, ef_ss, c_ss, c_rs, q_sem,
    ):
        i = lax.axis_index("mp")
        j = lax.axis_index("cand")
        me = i * n_cand + j
        user_side = i < half
        pool_side = jnp.logical_not(user_side)
        leader = i == half - 1
        follower = jnp.logical_not(leader)

        def remote(src, dst, ss, rs, where):
            return pltpu.make_async_remote_copy(
                src_ref=src, dst_ref=dst, send_sem=ss, recv_sem=rs, device_id=where, device_id_type=MESH
            )

        barrier = pltpu.get_barrier_semaphore()
        with scope("greet"):
            def greet(d, carry):
                pl.semaphore_signal(barrier, inc=1, device_id={"cand": lax.rem(j + d, n_cand)}, device_id_type=MESH)
                return carry

            @pl.when(leader)
            def _():
                lax.fori_loop(1, n_cand, greet, 0, unroll=n_cand <= 4)

            @pl.when(jnp.logical_and(follower, j > 0))
            def _():
                pl.semaphore_signal(barrier, inc=1, device_id={"cand": j - 1}, device_id_type=MESH)

            @pl.when(jnp.logical_and(follower, j < n_cand - 1))
            def _():
                pl.semaphore_signal(barrier, inc=1, device_id={"cand": j + 1}, device_id_type=MESH)

            @pl.when(user_side)
            def _():
                for d in range(1, n_mp):
                    pl.semaphore_signal(barrier, inc=1, device_id={"mp": lax.rem(i + d, n_mp)}, device_id_type=MESH)

            @pl.when(pool_side)
            def _():
                for d in range(1, half):
                    pl.semaphore_signal(
                        barrier, inc=1, device_id={"mp": half + lax.rem(i + d, half)}, device_id_type=MESH
                    )

        small_copies = [
            pltpu.make_async_copy(src, dst, small_sem.at[k])
            for k, (src, dst) in enumerate(
                (
                    (ids_hbm, ids_ref), (slot_hbm, slot_ref), (user_hbm, slots.at[j]), (b1_hbm, b1_ref),
                    (b2_hbm, b2_ref), (b3_hbm, b3_ref), (score_hbm, score_ref),
                )
            )
        ]
        m_start = pl.multiple_of(jnp.maximum(i - half, 0) * feat, 128)
        c_start = pl.multiple_of(jnp.maximum(j - first_pool_col, 0) * col, 128)
        pool_m_copy = pltpu.make_async_copy(pool_hbm.at[:, pl.ds(m_start, feat)], pool_m, w_sem.at[0])
        pool_c_copy = pltpu.make_async_copy(pool_hbm.at[:, pl.ds(c_start, col)], pool_c, w_sem.at[1])
        w1_copies = [
            pltpu.make_async_copy(w1_hbm.at[:, cut], w1_v.at[:, cut], w_sem.at[2 + c]) for c, cut in enumerate(cuts)
        ]
        w2_copy = pltpu.make_async_copy(w2_hbm, w2_v, w_sem.at[2 + n1])
        w3_copy = pltpu.make_async_copy(w3_hbm, w3_v, w_sem.at[3 + n1])
        col_pool = j >= first_pool_col
        with scope("loads"):
            for copy in small_copies[:3]:
                copy.start()

            @pl.when(pool_side)
            def _():
                pool_m_copy.start()

            for copy in w1_copies:
                copy.start()
            for copy in small_copies[3:]:
                copy.start()

            @pl.when(col_pool)
            def _():
                pool_c_copy.start()

            @pl.when(user_side)
            def _():
                w2_copy.start()

            end = jnp.logical_or(j == 0, j == n_cand - 1)
            inner = jnp.logical_not(end)
            nd = (j >= (n_cand + 1) // 2).astype(jnp.int32)

            @pl.when(end)
            def _():
                zr[nd] = jnp.zeros(zr.shape[1:], BF16)

        def build_onehot():
            with scope("onehot"):
                small_copies[0].wait()
                for u in range(users):
                    hot = (
                        lax.broadcasted_iota(jnp.int32, (pool_count, per_user), 0) == ids_ref[u : u + 1, :]
                    ).astype(F32).T
                    for p in range(n_mp):
                        first = p * block
                        if first // per_user == u:
                            off = first % per_user
                            onehot[p * block : (p + 1) * block, :] = hot[off : off + block].astype(BF16)

        def from_pool(dst, src, width):
            for c in range(0, width, 256):
                dst[:, c : c + 256] = jnp.dot(onehot[...], src[:, c : c + 256], preferred_element_type=F32).astype(BF16)

        def user_row(u):
            slot = slot_ref[0, u]
            row = slots[slot // slots_each].astype(F32)
            if slots_each > 1:
                pick = lax.broadcasted_iota(jnp.int32, row.shape, 0) == lax.rem(slot, slots_each)
                row = jnp.sum(jnp.where(pick, row, 0.0), axis=0, keepdims=True)
            return row

        def from_user(dst, index, width):
            row = urow[:, pl.ds(pl.multiple_of(index * width, 128), width)].astype(F32)
            for p in range(n_mp):
                u = user_of(p)
                dst[p * block : (p + 1) * block, :] = jnp.broadcast_to(row[u : u + 1], (block, width)).astype(BF16)

        def urow_copy(d):
            return remote(urow, urow, urow_ss.at[d], urow_rs.at[0], {"mp": lax.rem(i + d, half)})

        def user_copy(k):
            d = jnp.where(j < n_cand // 2, n_cand - k, k)
            return remote(user_hbm, slots.at[j], user_sem.at[0], user_sem.at[1], {"cand": lax.rem(j + d, n_cand)})

        def ucol_copy():
            return remote(ucol, ucol, ucol_sem.at[0], ucol_sem.at[1], {"mp": lax.rem(i + half, n_mp)})

        others = slots.at[pl.ds(0, n_cand - 1)]

        def from_all_users():
            remote(others, others, user_sem.at[0], user_sem.at[1], {"cand": j}).wait_recv()
            small_copies[1].wait()

        def bit_of(b):
            return lax.rem(i // (1 << b), 2)

        def partner(b):
            return i + (1 << b) * (1 - 2 * bit_of(b))

        lows = [0]
        for b in range(bits):
            lows.append(lows[b] + bit_of(b) * (rows >> (b + 1)))

        def seg(b):
            size = rows >> b
            if b == 0:
                return pl.ds(0, rows)
            return pl.ds(pl.multiple_of(lows[b], size), size)

        def other(b):
            size = rows >> (b + 1)
            start = lows[b] + (1 - bit_of(b)) * size
            return pl.ds(pl.multiple_of(start, size), size)

        def scatter_copy(c, b):
            size = rows >> (b + 1)
            return remote(
                send1.at[other(b), cuts[c]], recv1.at[b, pl.ds(0, size), cuts[c]], a_ss.at[b], a_rs.at[b, c], {"mp": partner(b)}
            )

        def across_copy(c):
            return remote(
                psum.at[seg(low), cuts[c]], psum.at[seg(low), cuts[c]], x_ss.at[0], x_rs.at[c], {"mp": lax.rem(i + half, n_mp)}
            )

        def gather_copy(c, b):
            return remote(
                psum.at[seg(b + 1), cuts[c]], psum.at[seg(b + 1), cuts[c]], g_ss.at[b], g_rs.at[b, c], {"mp": partner(b)}
            )

        def gather_wait(c, b):
            remote(
                psum.at[other(b), cuts[c]], psum.at[other(b), cuts[c]], g_ss.at[b], g_rs.at[b, c], {"mp": partner(b)}
            ).wait_recv()

        def spread(c):
            if low > 0:
                gather_copy(c, low - 1).start()

        def stage_a(c):
            w1_copies[c].wait()
            term = jnp.dot(base_mp[...], w1_v[:, cuts[c]], preferred_element_type=F32)
            if low > 0:
                acc1[:, cuts[c]] = term
                send1[:, cuts[c]] = term.astype(BF16)
            else:
                psum[:, cuts[c]] = term.astype(BF16)

        def stage_b(c):
            for b in range(low):
                scatter_copy(c, b).wait_recv()
                size = rows >> (b + 1)
                term = acc1[seg(b + 1), cuts[c]] + recv1[b, 0:size, cuts[c]].astype(F32)
                if b + 1 < low:
                    acc1[seg(b + 1), cuts[c]] = term
                    send1[seg(b + 1), cuts[c]] = term.astype(BF16)
                    scatter_copy(c, b + 1).start()
                else:
                    psum[seg(low), cuts[c]] = term.astype(BF16)
            across_copy(c).start()
            spread(c)

        def part_copy(c, d):
            return remote(ubuf.at[i, :, ucuts[c]], ubuf.at[i, :, ucuts[c]], u_ss.at[0], u_rs.at[c], {"mp": lax.rem(i + d, n_mp)})

        def part_wait(c, count):
            came = ubuf.at[pl.ds(0, count), :, ucuts[c]]
            remote(came, came, u_ss.at[0], u_rs.at[c], {"cand": j}).wait_recv()

        with scope("firstpart"):
            @pl.when(pool_side)
            def _():
                build_onehot()
                pool_m_copy.wait()
                from_pool(base_mp, pool_m, feat)

        neighbours = (j > 0).astype(jnp.int32) + (j < n_cand - 1).astype(jnp.int32)
        with scope("barrier"):
            pl.semaphore_wait(
                barrier,
                jnp.where(leader, n_cand - 1, neighbours) + jnp.where(user_side, half - 1, n_mp - 1),
            )

        with scope("layer1"):
            @pl.when(pool_side)
            def _():
                for d in range(half):
                    pl.semaphore_signal(ready.at[0], inc=1, device_id={"mp": d}, device_id_type=MESH)
                def pool_part(lag):
                    for c in range(n1 + lag):
                        if c < n1:
                            with scope(f"a{c}"):
                                stage_a(c)
                                if low > 0:
                                    scatter_copy(c, 0).start()
                            if c == n1 - 1:
                                w2_copy.start()
                        if c >= lag:
                            with scope(f"b{c - lag}"):
                                stage_b(c - lag)

                @pl.when(bit_of(0) == 0)
                def _():
                    pool_part(1)

                @pl.when(bit_of(0) != 0)
                def _():
                    pool_part(2)

            @pl.when(user_side)
            def _():
                @pl.when(leader)
                def _():
                    for k in range(1, n_cand):
                        user_copy(k).start()

                with scope("early"):
                    @pl.when(col_pool)
                    def _():
                        build_onehot()
                        pool_c_copy.wait()
                        from_pool(base_col, pool_c, col)

                    @pl.when(jnp.logical_not(col_pool))
                    def _():
                        small_copies[0].wait()

                    for copy in w1_copies:
                        copy.wait()
                    small_copies[2].wait()
                    pl.semaphore_wait(ready.at[0], half)
                with scope("users"):
                    @pl.when(leader)
                    def _():
                        from_all_users()
                        for u in range(users):
                            urow[u : u + 1, :] = user_row(u).astype(BF16)
                        for d in range(1, half):
                            urow_copy(d).start()

                    @pl.when(follower)
                    def _():
                        if half > 1:
                            urow_copy(0).wait_recv()
                        small_copies[1].wait()

                row = urow[:, pl.ds(pl.multiple_of(i * feat, 128), feat)]
                if users == 1:
                    lhs[...] = jnp.broadcast_to(row.astype(F32), lhs.shape).astype(BF16)
                else:
                    line = lax.broadcasted_iota(jnp.int32, lhs.shape, 0)
                    filled = jnp.zeros(lhs.shape, F32)
                    for u in range(users):
                        filled = jnp.where(line == u, row[u : u + 1].astype(F32), filled)
                    lhs[...] = filled.astype(BF16)
                for c, cut in enumerate(ucuts):
                    with scope(f"um{c}"):
                        term = jnp.dot(lhs[...], w1_v[:, cut], preferred_element_type=F32)
                        ubuf[i, :, cut] = term[0:users]
                        for d in range(n_mp - 1, 0, -1):
                            part_copy(c, d).start()
                    if c == 0:
                        @pl.when(jnp.logical_not(col_pool))
                        def _():
                            ucol[...] = urow[:, pl.ds(pl.multiple_of(j * col, 128), col)]
                            ucol_copy().start()

        def take_across(c):
            @pl.when(user_side)
            def _():
                with scope(f"across{c}"):
                    across_copy(c).wait_recv()
                spread(c)

        ahead = min(2, n1)
        with scope("bases"):
            w3_copy.start()

            for c in range(ahead):
                take_across(c)

            @pl.when(user_side)
            def _():
                from_user(base_mp, i, feat)

            @pl.when(jnp.logical_and(col_pool, pool_side))
            def _():
                pool_c_copy.wait()
                from_pool(base_col, pool_c, col)

            @pl.when(jnp.logical_not(col_pool))
            def _():
                @pl.when(pool_side)
                def _():
                    ucol_copy().wait_recv()

                for p in range(n_mp):
                    u = user_of(p)
                    value = ucol[u : u + 1, :].astype(F32)
                    base_col[p * block : (p + 1) * block, :] = jnp.broadcast_to(value, (block, col)).astype(BF16)

            for copy in small_copies[3:]:
                copy.wait()

            @pl.when(pool_side)
            def _():
                for copy in small_copies[1:3]:
                    copy.wait()

        def first_cross(c):
            with scope(f"gw{c}"):
                for b in range(low - 1, -1, -1):
                    gather_wait(c, b)
                    if b > 0:
                        gather_copy(c, b - 1).start()
            for u, ucut in enumerate(ucuts):
                if ucut.start != cuts[c].start:
                    continue
                with scope(f"pw{u}"):
                    @pl.when(user_side)
                    def _():
                        if half > 1:
                            part_wait(u, half - 1)

                    @pl.when(pool_side)
                    def _():
                        part_wait(u, half)

            cols = cuts[c]
            added = b1_ref[:, cols]
            for src in range(half):
                added = added + ubuf[src, :, cols]
            for p in range(n_mp):
                r = slice(p * block, (p + 1) * block)
                u = user_of(p)
                base = base_col[r, cols].astype(F32)
                cross1[r, cols] = (base * (psum[r, cols].astype(F32) + added[u : u + 1]) + base).astype(BF16)

        toward = 1 - 2 * nd

        def z_copy(g, n, way, src, step):
            at = (halves[g], zcuts[g][n])
            return remote(
                src.at[at], zr.at[(way,) + at], z_ss.at[way], z_rs.at[way, place[g, n]], {"cand": j + step}
            )

        def z_wait(g, n, way):
            at = (halves[g], zcuts[g][n])
            remote(q_send.at[at], zr.at[(way,) + at], z_ss.at[way], z_rs.at[way, place[g, n]], {"cand": j}).wait_recv()

        def first_out(cols):
            last = cuts[n1 - 1]
            term = jnp.dot(cross1[:, last], w2_v[last, cols], preferred_element_type=F32)
            if n1 > 1:
                term = acc2[:, cols] + term
            owner = (j == i * ratio + cols.start // col).astype(F32)
            inside = cols.start % col
            carried = cross1[:, inside : inside + cols.stop - cols.start].astype(F32)
            term = base_mp[:, cols].astype(F32) * (term + owner * b2_ref[:, cols]) + owner * carried
            q_send[:, cols] = term.astype(BF16)

        for c in range(n1):
            first_cross(c)
            if c + ahead < n1:
                take_across(c + ahead)
            if c == 0:
                w2_copy.wait()
            if c < n1 - 1:
                with scope(f"l2_{c}"):
                    term = jnp.dot(cross1[:, cuts[c]], w2_v[cuts[c], :], preferred_element_type=F32)
                    acc2[...] = term if c == 0 else acc2[...] + term
        even = bit_of(0) == 0
        odd = jnp.logical_not(even)
        detour = jnp.logical_and(even, j == n_cand - 1) if n_cand > 2 else None

        def detour_copy(g, n):
            at = (halves[g], zcuts[g][n])
            return remote(
                q_send.at[at], ze.at[at], z_ss.at[1], ze_rs.at[place[g, n]], {"mp": i + 1, "cand": j - 1}
            )

        def first_send(g, ns):
            @pl.when(end if detour is None else jnp.logical_and(end, jnp.logical_not(detour)))
            def _():
                for n in ns:
                    z_copy(g, n, nd, q_send, toward).start()

            if detour is not None:
                @pl.when(detour)
                def _():
                    for n in ns:
                        detour_copy(g, n).start()

        def lend_copy(s):
            cols = slice(zcuts[0][s].start, zcuts[0][min(s + 1, len(zcuts[0]) - 1)].stop)
            return remote(q_send.at[:, cols], qe.at[:, cols], qe_ss.at[0], qe_rs.at[s // 2], {"mp": i + 1 - 2 * bit_of(0)})

        for s in range(0, len(zcuts[0]), 2):
            with scope(f"q{s}"):
                for cols in zcuts[0][s : s + 2]:
                    first_out(cols)
                first_send(0, range(s, min(s + 2, len(zcuts[0]))))

                @pl.when(jnp.logical_and(inner, even))
                def _():
                    lend_copy(s).start()

        for g in range(1, len(zcuts)):
            first_send(g, range(len(zcuts[g])))

        def pass_on(g, n, way, step):
            at = (halves[g], zcuts[g][n])
            zs[(way,) + at] = (zr[(way,) + at].astype(F32) + q_send[at].astype(F32)).astype(BF16)
            z_copy(g, n, way, zs.at[way], step).start()

        def near(g, n):
            with scope(f"near{g}_{n}"):
                z_wait(g, n, nd)
            pass_on(g, n, nd, toward)

        def far(g, n, passing):
            with scope(f"far{g}_{n}"):
                z_wait(g, n, 1 - nd)
            if passing:
                pass_on(g, n, 1 - nd, -toward)

        def relay(g, n):
            at = (halves[g], zcuts[g][n])
            k = place[g, n]
            with scope(f"relay{g}_{n}"):
                remote(ze.at[at], ze.at[at], ef_ss.at[0], ze_rs.at[k], {"cand": j}).wait_recv()
            if g == 0 and n % 2 == 0:
                lend_copy(n).wait_recv()
            zf[at] = (ze[at].astype(F32) + qe[at].astype(F32)).astype(BF16)

            @pl.when(j > 1)
            def _():
                remote(zf.at[at], ze.at[at], ef_ss.at[0], ze_rs.at[k], {"cand": j - 1}).start()

            @pl.when(j == 1)
            def _():
                remote(
                    zf.at[at], zr.at[(1,) + at], ef_ss.at[0], z_rs.at[1, k], {"mp": i - 1, "cand": j - 1}
                ).start()

            remote(ze.at[at], zr.at[(1,) + at], ef_ss.at[1], z_rs.at[1, k], {"mp": i - 1}).start()

        def third(g, n):
            cols = zcuts[g][n]
            r = halves[g]
            value = (
                q_send[r, cols].astype(F32) + zr[0, r, cols].astype(F32) + zr[1, r, cols].astype(F32)
            ).astype(BF16)
            x3[r, cols] = value
            if g == 0 and n == 0:
                w3_copy.wait()
            term = jnp.dot(value, w3_v[cols, :], preferred_element_type=F32)
            acc3[r, :] = term if n == 0 else acc3[r, :] + term

        def last_copy(c, peer):
            r = pl.ds(pl.multiple_of(peer * block, block), block)
            cols = slice(c * cw3, (c + 1) * cw3)
            return remote(send3.at[r, cols], recv3.at[i, :, cols], c_ss.at[0], c_rs.at[c], {"mp": peer})

        owner3 = (i == j // ratio).astype(F32)

        def q_copy(g, peer, dj):
            return remote(
                q_mine.at[g], q_all.at[me], q_sem.at[0], q_sem.at[1],
                {"mp": peer, "cand": lax.rem(j + dj, n_cand)},
            )

        def score_row(lanes, count):
            if q_width == 128:
                total = jnp.sum(lanes, axis=1, keepdims=True)
                row = lax.broadcasted_iota(jnp.int32, lanes.shape, 0)
                lane = lax.broadcasted_iota(jnp.int32, lanes.shape, 1)
                return jnp.sum(jnp.where(row == lane, total, 0.0), axis=0, keepdims=True)
            q_rows[0:count, :] = lanes
            return jnp.sum(q_rows[...].T, axis=0, keepdims=True)

        def epilogue(g):
            r = halves[g]
            for c in range(n3):
                cols = slice(c * cw3, (c + 1) * cw3)
                if ratio == 1:
                    carried = x3[r, cols]
                else:
                    carried = x3[r, pl.ds(pl.multiple_of(lax.rem(j, ratio) * col + c * cw3, 128), cw3)]
                term = (
                    base_col[r, cols].astype(F32) * (acc3[r, cols] + owner3 * b3_ref[:, cols])
                    + owner3 * carried.astype(F32)
                )
                acc3[r, cols] = term
                send3[r, cols] = term.astype(BF16)
            for peer in range(*spans[g]):
                @pl.when(i != peer)
                def _():
                    for c in range(n3):
                        last_copy(c, peer).start()

            count = r.stop - r.start
            lanes = jnp.zeros((count, 128), F32)
            for k in range(0, col, 128):
                lanes = lanes + acc3[r, k : k + 128] * score_ref[k : k + 128].astype(F32).reshape(1, 128)
            q_mine[g] = score_row(lanes, count)

            def each(dj, carry):
                for peer in range(*spans[g]):
                    q_copy(g, peer, dj).start()
                return carry

            if n_cand <= 4:
                for dj in sorted(range(1, n_cand), key=lambda d: -min(d, n_cand - d)):
                    each(dj, 0)
            else:
                lax.fori_loop(1, n_cand, each, 0)
            for peer in range(*spans[g]):
                @pl.when(i != peer)
                def _():
                    q_copy(g, peer, 0).start()

                @pl.when(i == peer)
                def _():
                    q_all[me] = q_mine[g]

        if q_width > 128:
            q_rows[...] = jnp.zeros(q_rows.shape, F32)

        def stream(skew, nears, passing, relays):
            ready_at = len(events) - skew if nears else 0
            for s in range(len(events) + skew):
                if nears and s < len(events):
                    near(*events[s])
                    if relays == 1:
                        relay(*events[s])
                if s < skew:
                    continue
                g, n = events[s - skew]
                far(g, n, passing)
                if relays == 2:
                    relay(g, n)
                if passing and not nears:
                    z_wait(g, n, nd)
                with scope(f"third{g}_{n}"):
                    third(g, n)
                for done in range(len(spans)):
                    last = place[done, len(zcuts[done]) - 1]
                    if s - skew == max(last, min(ready_at, len(events) - 1)):
                        with scope(f"epi{done}"):
                            epilogue(done)

        @pl.when(end)
        def _():
            stream(0, False, False, 0)

        if n_cand > 2:
            left = nd == 0

            @pl.when(jnp.logical_and(inner, jnp.logical_and(odd, left)))
            def _():
                stream(min(11, len(events)), True, True, 2)

            @pl.when(jnp.logical_and(inner, jnp.logical_and(odd, jnp.logical_not(left))))
            def _():
                stream(min(2, len(events)), True, True, 1)

            @pl.when(jnp.logical_and(inner, jnp.logical_and(even, left)))
            def _():
                stream(min(11, len(events)), True, False, 0)

            @pl.when(jnp.logical_and(inner, jnp.logical_and(even, jnp.logical_not(left))))
            def _():
                stream(0, False, True, 0)

        mine = pl.ds(pl.multiple_of(i * block, block), block)
        for c in range(n3):
            cols = slice(c * cw3, (c + 1) * cw3)
            with scope(f"last{c}"):
                came = recv3.at[pl.ds(0, n_mp - 1), :, cols]
                remote(came, came, c_ss.at[0], c_rs.at[c], {"mp": i}).wait_recv()
            term = acc3[mine, cols]
            for d in range(1, n_mp):
                term = term + recv3[lax.rem(i - d + n_mp, n_mp), :, cols].astype(F32)
            out_ref[:, cols] = term.astype(BF16)

        with scope("qwait"):
            rest = q_all.at[pl.ds(0, group - 1)]
            remote(rest, rest, q_sem.at[0], q_sem.at[1], {"cand": j}).wait_recv()
            total = jnp.sum(q_all[...], axis=0)
            for lo, hi in spans:
                for k in range(lo, hi):
                    @pl.when(i == k)
                    def _():
                        logit_ref[...] = total[:, (k - lo) * block : (k - lo + 1) * block]

        def sent(ref, sem):
            remote(ref, ref, sem, sem, {"cand": j}).wait_send()

        with scope("sent"):
            @pl.when(pool_side)
            def _():
                for b in range(low):
                    sent(recv1.at[b, pl.ds(0, rows >> (b + 1)), :], a_ss.at[b])
                sent(psum.at[seg(low), :], x_ss.at[0])

            @pl.when(user_side)
            def _():
                @pl.when(leader)
                def _():
                    sent(others, user_sem.at[0])
                    for d in range(1, half):
                        sent(urow, urow_ss.at[d])

                @pl.when(jnp.logical_not(col_pool))
                def _():
                    sent(ucol, ucol_sem.at[0])

                sent(ubuf.at[pl.ds(0, n_mp - 1)], u_ss.at[0])

            for b in range(low):
                sent(psum.at[seg(b + 1), :], g_ss.at[b])
            @pl.when(end)
            def _():
                sent(q_send, z_ss.at[nd])

            @pl.when(inner)
            def _():
                sent(q_send, z_ss.at[0])

            @pl.when(jnp.logical_and(inner, odd))
            def _():
                for sem in (z_ss.at[1], ef_ss.at[0], ef_ss.at[1]):
                    sent(q_send, sem)

            @pl.when(jnp.logical_and(inner, even))
            def _():
                sent(q_send, qe_ss.at[0])

            sent(recv3.at[pl.ds(0, n_mp - 1)], c_ss.at[0])
            sent(rest, q_sem.at[0])

    return kernel


def solution(mesh):
    n_mp, n_cand = mesh.shape["mp"], mesh.shape["cand"]

    def body(
        user_feats, user_slot, cand_pool, cand_ids, first_weight, first_bias,
        second_weight, second_bias, third_weight, third_bias, score_weight,
    ):
        slots_each, half_width = user_feats.shape
        users, per_user = cand_ids.shape
        rows = users * per_user
        pool_count = cand_pool.shape[0]
        feat, col = first_weight.shape
        wide = min(512, col)
        ucuts = [slice(k, k + wide) for k in range(0, col, wide)]
        cuts = list(ucuts)
        half = n_mp // 2
        spans = [(0, half), (half, n_mp)]
        if half > 1:
            spans[1:] = [(half, half + half // 2), (half + half // 2, n_mp)]
        zcuts = []
        for lo, hi in spans:
            step = min(256 * half // (hi - lo), col, feat)
            zcuts.append([slice(k, k + step) for k in range(0, feat, step)])
        if step > 128:
            zcuts[-1][-1:] = [slice(feat - step, feat - step // 2), slice(feat - step // 2, feat)]
        n1 = len(cuts)
        n3 = max(1, col // 512)
        lhs_rows = -(-users // 16) * 16
        bits = n_mp.bit_length() - 1
        low = max(1, bits - 1)
        block = rows // n_mp
        group = n_mp * n_cand
        shapes = (rows, per_user, users, slots_each, half_width, pool_count, feat, col, cuts, ucuts, zcuts, spans, n3)
        vmem = pl.BlockSpec(memory_space=pltpu.VMEM)
        hbm = pl.BlockSpec(memory_space=pl.ANY)
        dma = pltpu.SemaphoreType.DMA
        crossed, logits = pl.pallas_call(
            make_kernel(n_mp, n_cand, shapes),
            out_shape=(
                pltpu.VMEM((block, col), BF16),
                pltpu.VMEM((1, block), F32),
            ),
            in_specs=[hbm] * 11,
            out_specs=(vmem, vmem),
            scratch_shapes=[
                pltpu.SMEM((1, users), jnp.int32),
                pltpu.VMEM((users, per_user), jnp.int32),
                pltpu.VMEM((1, col), F32),
                pltpu.VMEM((1, feat), F32),
                pltpu.VMEM((1, col), F32),
                pltpu.VMEM((col,), BF16),
                dma((7,)),
                pltpu.VMEM((n_cand, slots_each, half_width), BF16),
                pltpu.VMEM((users, half_width), BF16),
                pltpu.VMEM((users, col), BF16),
                pltpu.VMEM((pool_count, feat), BF16),
                pltpu.VMEM((pool_count, col), BF16),
                pltpu.VMEM((feat, col), BF16),
                pltpu.VMEM((col, feat), BF16),
                pltpu.VMEM((feat, col), BF16),
                pltpu.VMEM((rows, pool_count), BF16),
                pltpu.VMEM((rows, feat), BF16),
                pltpu.VMEM((rows, col), BF16),
                pltpu.VMEM((lhs_rows, feat), BF16),
                pltpu.VMEM((rows, col), F32),
                pltpu.VMEM((rows, col), BF16),
                pltpu.VMEM((low, rows // 2, col), BF16),
                pltpu.VMEM((rows, col), BF16),
                pltpu.VMEM((n_mp, users, col), F32),
                pltpu.VMEM((rows, col), BF16),
                pltpu.VMEM((rows, feat), F32),
                pltpu.VMEM((rows, feat), BF16),
                pltpu.VMEM((2, rows, feat), BF16),
                pltpu.VMEM((2, rows, feat), BF16),
                pltpu.VMEM((rows, feat), BF16),
                pltpu.VMEM((rows, feat), BF16),
                pltpu.VMEM((rows, feat), BF16),
                pltpu.VMEM((rows, feat), BF16),
                pltpu.VMEM((rows, col), F32),
                pltpu.VMEM((rows, col), BF16),
                pltpu.VMEM((n_mp, block, col), BF16),
                pltpu.VMEM((max(rows // 2, 128), 128), F32),
                pltpu.VMEM((len(spans), 1, max(rows // 2, 128)), F32),
                pltpu.VMEM((group, 1, max(rows // 2, 128)), F32),
                dma((4 + n1,)),
                dma((2,)),
                dma((half,)),
                dma((1,)),
                dma((2,)),
                pltpu.SemaphoreType.REGULAR((1,)),
                dma((low,)),
                dma((low, n1)),
                dma((1,)),
                dma((n1,)),
                dma((low,)),
                dma((low, n1)),
                dma((1,)),
                dma((len(ucuts),)),
                dma((2,)),
                dma((2, sum(len(part) for part in zcuts))),
                dma((sum(len(part) for part in zcuts),)),
                dma((1,)),
                dma((-(-len(zcuts[0]) // 2),)),
                dma((2,)),
                dma((1,)),
                dma((n3,)),
                dma((2,)),
            ],
            compiler_params=pltpu.CompilerParams(
                collective_id=0, has_side_effects=True, vmem_limit_bytes=67043328 - 3000 * 1024
            ),
        )(
            user_feats, user_slot.reshape(1, -1), cand_pool, cand_ids, first_weight, first_bias.reshape(1, -1),
            second_weight, second_bias.reshape(1, -1), third_weight, third_bias.reshape(1, -1),
            score_weight,
        )
        crossed, logits = pl.pallas_call(
            hand_on,
            out_shape=(
                jax.ShapeDtypeStruct((block, col), BF16),
                jax.ShapeDtypeStruct((1, block), F32),
            ),
            in_specs=[vmem, vmem],
            out_specs=(hbm, hbm),
            scratch_shapes=[dma((2,))],
            compiler_params=pltpu.CompilerParams(vmem_limit_bytes=1024 * 1024),
        )(crossed, logits)
        return crossed, logits.reshape(-1)

    in_specs = (
        P(("groups", "cand"), None),
        P("groups"),
        P("groups", None),
        P("groups", None),
        P("mp", "cand"),
        P("cand"),
        P("cand", "mp"),
        P("mp"),
        P("mp", "cand"),
        P("cand"),
        P("cand"),
    )
    out_specs = (P(("groups", "mp"), "cand"), P(("groups", "mp")))
    return jax.shard_map(body, mesh=mesh, in_specs=in_specs, out_specs=out_specs, check_vma=False)
```

```python
import contextlib

import jax
import jax.numpy as jnp
from jax import lax
from jax.experimental import pallas as pl
from jax.experimental.pallas import tpu as pltpu
from jax.sharding import PartitionSpec as P

MESH = pl.DeviceIdType.MESH
F32 = jnp.float32
BF16 = jnp.bfloat16


def scope(name):
    return contextlib.nullcontext()


def hand_on(crossed_ref, logit_ref, crossed_hbm, logit_hbm, sem):
    copies = [
        pltpu.make_async_copy(crossed_ref, crossed_hbm, sem.at[0]),
        pltpu.make_async_copy(logit_ref, logit_hbm, sem.at[1]),
    ]
    for copy in copies:
        copy.start()
    for copy in copies:
        copy.wait()


def make_kernel(n_mp, n_cand, shapes):
    rows, per_user, users, slots_each, half_width, pool_count, feat, col, cuts, ucuts, zcuts, spans, n3 = shapes
    cw3 = col // n3
    n1 = len(cuts)
    bits = n_mp.bit_length() - 1
    low = bits - 1
    half = n_mp // 2
    block = rows // n_mp
    ratio = feat // col
    group = n_mp * n_cand
    halves = [slice(lo * block, hi * block) for lo, hi in spans]
    events = [(g, n) for g in range(len(spans)) for n in range(len(zcuts[g]))]
    place = {event: k for k, event in enumerate(events)}
    q_width = max([128] + [r.stop - r.start for r in halves])
    first_pool_col = half_width // col

    def user_of(p):
        return (p * block) // per_user

    def kernel(
        user_hbm, slot_hbm, pool_hbm, ids_hbm, w1_hbm, b1_hbm, w2_hbm, b2_hbm, w3_hbm, b3_hbm, score_hbm,
        out_ref, logit_ref,
        slot_ref, ids_ref, b1_ref, b2_ref, b3_ref, score_ref, small_sem, slots, urow, ucol, pool_m, pool_c, w1_v, w2_v, w3_v,
        onehot, base_mp, base_col, lhs, acc1, send1, recv1, psum, ubuf, cross1, acc2, q_send, zr, zs, ze, zf, qe, x3, acc3, send3, recv3,
        q_rows, q_mine, q_all,
        w_sem, user_sem, urow_ss, urow_rs, ucol_sem, ready, a_ss, a_rs, x_ss, x_rs, g_ss, g_rs, u_ss, u_rs, z_ss, z_rs, ze_rs, qe_ss, qe_rs, ef_ss, c_ss, c_rs, q_sem,
    ):
        i = lax.axis_index("mp")
        j = lax.axis_index("cand")
        me = i * n_cand + j
        user_side = i < half
        pool_side = jnp.logical_not(user_side)
        leader = i == half - 1
        follower = jnp.logical_not(leader)

        def remote(src, dst, ss, rs, where):
            return pltpu.make_async_remote_copy(
                src_ref=src, dst_ref=dst, send_sem=ss, recv_sem=rs, device_id=where, device_id_type=MESH
            )

        barrier = pltpu.get_barrier_semaphore()
        with scope("greet"):
            def greet(d, carry):
                pl.semaphore_signal(barrier, inc=1, device_id={"cand": lax.rem(j + d, n_cand)}, device_id_type=MESH)
                return carry

            @pl.when(leader)
            def _():
                lax.fori_loop(1, n_cand, greet, 0, unroll=n_cand <= 4)

            @pl.when(jnp.logical_and(follower, j > 0))
            def _():
                pl.semaphore_signal(barrier, inc=1, device_id={"cand": j - 1}, device_id_type=MESH)

            @pl.when(jnp.logical_and(follower, j < n_cand - 1))
            def _():
                pl.semaphore_signal(barrier, inc=1, device_id={"cand": j + 1}, device_id_type=MESH)

            @pl.when(user_side)
            def _():
                for d in range(1, n_mp):
                    pl.semaphore_signal(barrier, inc=1, device_id={"mp": lax.rem(i + d, n_mp)}, device_id_type=MESH)

            @pl.when(pool_side)
            def _():
                for d in range(1, half):
                    pl.semaphore_signal(
                        barrier, inc=1, device_id={"mp": half + lax.rem(i + d, half)}, device_id_type=MESH
                    )

        small_copies = [
            pltpu.make_async_copy(src, dst, small_sem.at[k])
            for k, (src, dst) in enumerate(
                (
                    (ids_hbm, ids_ref), (slot_hbm, slot_ref), (user_hbm, slots.at[j]), (b1_hbm, b1_ref),
                    (b2_hbm, b2_ref), (b3_hbm, b3_ref), (score_hbm, score_ref),
                )
            )
        ]
        m_start = pl.multiple_of(jnp.maximum(i - half, 0) * feat, 128)
        c_start = pl.multiple_of(jnp.maximum(j - first_pool_col, 0) * col, 128)
        pool_m_copy = pltpu.make_async_copy(pool_hbm.at[:, pl.ds(m_start, feat)], pool_m, w_sem.at[0])
        pool_c_copy = pltpu.make_async_copy(pool_hbm.at[:, pl.ds(c_start, col)], pool_c, w_sem.at[1])
        w1_copies = [
            pltpu.make_async_copy(w1_hbm.at[:, cut], w1_v.at[:, cut], w_sem.at[2 + c]) for c, cut in enumerate(cuts)
        ]
        w2_copy = pltpu.make_async_copy(w2_hbm, w2_v, w_sem.at[2 + n1])
        w3_copy = pltpu.make_async_copy(w3_hbm, w3_v, w_sem.at[3 + n1])
        col_pool = j >= first_pool_col
        with scope("loads"):
            for copy in small_copies[:3]:
                copy.start()

            @pl.when(pool_side)
            def _():
                pool_m_copy.start()

            for copy in w1_copies:
                copy.start()
            for copy in small_copies[3:]:
                copy.start()

            @pl.when(col_pool)
            def _():
                pool_c_copy.start()

            @pl.when(user_side)
            def _():
                w2_copy.start()

            end = jnp.logical_or(j == 0, j == n_cand - 1)
            inner = jnp.logical_not(end)
            nd = (j >= (n_cand + 1) // 2).astype(jnp.int32)

            @pl.when(end)
            def _():
                zr[nd] = jnp.zeros(zr.shape[1:], BF16)

        def build_onehot():
            with scope("onehot"):
                small_copies[0].wait()
                for u in range(users):
                    hot = (
                        lax.broadcasted_iota(jnp.int32, (pool_count, per_user), 0) == ids_ref[u : u + 1, :]
                    ).astype(F32).T
                    for p in range(n_mp):
                        first = p * block
                        if first // per_user == u:
                            off = first % per_user
                            onehot[p * block : (p + 1) * block, :] = hot[off : off + block].astype(BF16)

        def from_pool(dst, src, width):
            for c in range(0, width, 256):
                dst[:, c : c + 256] = jnp.dot(onehot[...], src[:, c : c + 256], preferred_element_type=F32).astype(BF16)

        def user_row(u):
            slot = slot_ref[0, u]
            row = slots[slot // slots_each].astype(F32)
            if slots_each > 1:
                pick = lax.broadcasted_iota(jnp.int32, row.shape, 0) == lax.rem(slot, slots_each)
                row = jnp.sum(jnp.where(pick, row, 0.0), axis=0, keepdims=True)
            return row

        def from_user(dst, index, width):
            row = urow[:, pl.ds(pl.multiple_of(index * width, 128), width)].astype(F32)
            for p in range(n_mp):
                u = user_of(p)
                dst[p * block : (p + 1) * block, :] = jnp.broadcast_to(row[u : u + 1], (block, width)).astype(BF16)

        def urow_copy(d):
            return remote(urow, urow, urow_ss.at[d], urow_rs.at[0], {"mp": lax.rem(i + d, half)})

        def user_copy(k):
            d = jnp.where(j < n_cand // 2, n_cand - k, k)
            return remote(user_hbm, slots.at[j], user_sem.at[0], user_sem.at[1], {"cand": lax.rem(j + d, n_cand)})

        def ucol_copy():
            return remote(ucol, ucol, ucol_sem.at[0], ucol_sem.at[1], {"mp": lax.rem(i + half, n_mp)})

        others = slots.at[pl.ds(0, n_cand - 1)]

        def from_all_users():
            remote(others, others, user_sem.at[0], user_sem.at[1], {"cand": j}).wait_recv()
            small_copies[1].wait()

        def bit_of(b):
            return lax.rem(i // (1 << b), 2)

        def partner(b):
            return i + (1 << b) * (1 - 2 * bit_of(b))

        def ones(b):
            return lax.rem(i, 1 << b) == (1 << b) - 1

        root = ones(low)
        leaf = jnp.logical_not(root)

        def tree_copy(c, b):
            return remote(
                send1.at[:, cuts[c]], recv1.at[b, :, cuts[c]], a_ss.at[b], a_rs.at[b, c], {"mp": partner(b)}
            )

        def across_copy(c):
            return remote(
                psum.at[:, cuts[c]], psum.at[:, cuts[c]], x_ss.at[0], x_rs.at[c], {"mp": lax.rem(i + half, n_mp)}
            )

        def spread_copy(c, b):
            return remote(psum.at[:, cuts[c]], psum.at[:, cuts[c]], g_ss.at[b], g_rs.at[c], {"mp": partner(b)})

        def reduce(c, b):
            cut = cuts[c]
            if b == low:
                psum[:, cut] = acc1[:, cut].astype(BF16)
                hand_out(c)
                return

            @pl.when(bit_of(b) == 0)
            def _():
                send1[:, cut] = acc1[:, cut].astype(BF16)
                tree_copy(c, b).start()

            @pl.when(bit_of(b) != 0)
            def _():
                tree_copy(c, b).wait_recv()
                acc1[:, cut] = acc1[:, cut] + recv1[b, :, cut].astype(F32)
                reduce(c, b + 1)

        def hand_out(c):
            across_copy(c).start()
            for b in range(low - 1, -1, -1):
                spread_copy(c, b).start()

        def stage_a(c, sends):
            w1_copies[c].wait()
            term = jnp.dot(base_mp[...], w1_v[:, cuts[c]], preferred_element_type=F32)
            if sends:
                send1[:, cuts[c]] = term.astype(BF16)
                tree_copy(c, 0).start()
            else:
                acc1[:, cuts[c]] = term

        def stage_b(c):
            if low == 1:
                cut = cuts[c]
                tree_copy(c, 0).wait_recv()
                psum[:, cut] = (acc1[:, cut] + recv1[0, :, cut].astype(F32)).astype(BF16)
                hand_out(c)
            else:
                reduce(c, 0)

        def part_copy(c, d):
            return remote(ubuf.at[i, :, ucuts[c]], ubuf.at[i, :, ucuts[c]], u_ss.at[0], u_rs.at[c], {"mp": lax.rem(i + d, n_mp)})

        def part_wait(c, count):
            came = ubuf.at[pl.ds(0, count), :, ucuts[c]]
            remote(came, came, u_ss.at[0], u_rs.at[c], {"cand": j}).wait_recv()

        with scope("firstpart"):
            @pl.when(pool_side)
            def _():
                build_onehot()
                pool_m_copy.wait()
                from_pool(base_mp, pool_m, feat)

        neighbours = (j > 0).astype(jnp.int32) + (j < n_cand - 1).astype(jnp.int32)
        with scope("barrier"):
            pl.semaphore_wait(
                barrier,
                jnp.where(leader, n_cand - 1, neighbours) + jnp.where(user_side, half - 1, n_mp - 1),
            )

        with scope("layer1"):
            @pl.when(pool_side)
            def _():
                for d in range(half):
                    pl.semaphore_signal(ready.at[0], inc=1, device_id={"mp": d}, device_id_type=MESH)
                def pool_part(sends):
                    lag = n1 if sends else 2
                    for c in range(n1 + lag):
                        if c < n1:
                            with scope(f"a{c}"):
                                stage_a(c, sends)
                            if c == n1 - 1:
                                w2_copy.start()
                        if c >= lag and not sends:
                            with scope(f"b{c - lag}"):
                                stage_b(c - lag)

                if low > 0:
                    @pl.when(bit_of(0) == 0)
                    def _():
                        pool_part(True)

                    @pl.when(bit_of(0) != 0)
                    def _():
                        pool_part(False)
                else:
                    pool_part(False)

            @pl.when(user_side)
            def _():
                @pl.when(leader)
                def _():
                    for k in range(1, n_cand):
                        user_copy(k).start()

                with scope("early"):
                    @pl.when(col_pool)
                    def _():
                        build_onehot()
                        pool_c_copy.wait()
                        from_pool(base_col, pool_c, col)

                    @pl.when(jnp.logical_not(col_pool))
                    def _():
                        small_copies[0].wait()

                    for copy in w1_copies:
                        copy.wait()
                    small_copies[2].wait()
                    pl.semaphore_wait(ready.at[0], half)
                with scope("users"):
                    @pl.when(leader)
                    def _():
                        from_all_users()
                        for u in range(users):
                            urow[u : u + 1, :] = user_row(u).astype(BF16)
                        for d in range(1, half):
                            urow_copy(d).start()

                    @pl.when(follower)
                    def _():
                        if half > 1:
                            urow_copy(0).wait_recv()
                        small_copies[1].wait()

                row = urow[:, pl.ds(pl.multiple_of(i * feat, 128), feat)]
                if users == 1:
                    lhs[...] = jnp.broadcast_to(row.astype(F32), lhs.shape).astype(BF16)
                else:
                    line = lax.broadcasted_iota(jnp.int32, lhs.shape, 0)
                    filled = jnp.zeros(lhs.shape, F32)
                    for u in range(users):
                        filled = jnp.where(line == u, row[u : u + 1].astype(F32), filled)
                    lhs[...] = filled.astype(BF16)
                for c, cut in enumerate(ucuts):
                    with scope(f"um{c}"):
                        term = jnp.dot(lhs[...], w1_v[:, cut], preferred_element_type=F32)
                        ubuf[i, :, cut] = term[0:users]
                        for d in range(n_mp - 1, 0, -1):
                            part_copy(c, d).start()
                    if c == 0:
                        @pl.when(jnp.logical_not(col_pool))
                        def _():
                            ucol[...] = urow[:, pl.ds(pl.multiple_of(j * col, 128), col)]
                            ucol_copy().start()

        def take_across(c):
            @pl.when(jnp.logical_and(user_side, root))
            def _():
                with scope(f"across{c}"):
                    across_copy(c).wait_recv()
                for b in range(low - 1, -1, -1):
                    spread_copy(c, b).start()

        ahead = 1
        with scope("bases"):
            w3_copy.start()

            for c in range(ahead):
                take_across(c)

            @pl.when(user_side)
            def _():
                from_user(base_mp, i, feat)

            @pl.when(jnp.logical_and(col_pool, pool_side))
            def _():
                pool_c_copy.wait()
                from_pool(base_col, pool_c, col)

            @pl.when(jnp.logical_not(col_pool))
            def _():
                @pl.when(pool_side)
                def _():
                    ucol_copy().wait_recv()

                for p in range(n_mp):
                    u = user_of(p)
                    value = ucol[u : u + 1, :].astype(F32)
                    base_col[p * block : (p + 1) * block, :] = jnp.broadcast_to(value, (block, col)).astype(BF16)

            for copy in small_copies[3:]:
                copy.wait()

            @pl.when(pool_side)
            def _():
                for copy in small_copies[1:3]:
                    copy.wait()

        def first_cross(c):
            if low > 0:
                @pl.when(leaf)
                def _():
                    with scope(f"gw{c}"):
                        spread_copy(c, 0).wait_recv()

                for b in range(low - 2, -1, -1):
                    @pl.when(jnp.logical_and(leaf, ones(b + 1)))
                    def _():
                        spread_copy(c, b).start()

            for u, ucut in enumerate(ucuts):
                if ucut.start != cuts[c].start:
                    continue
                with scope(f"pw{u}"):
                    @pl.when(user_side)
                    def _():
                        if half > 1:
                            part_wait(u, half - 1)

                    @pl.when(pool_side)
                    def _():
                        part_wait(u, half)

            cols = cuts[c]
            added = b1_ref[:, cols]
            for src in range(half):
                added = added + ubuf[src, :, cols]
            for p in range(n_mp):
                r = slice(p * block, (p + 1) * block)
                u = user_of(p)
                base = base_col[r, cols].astype(F32)
                cross1[r, cols] = (base * (psum[r, cols].astype(F32) + added[u : u + 1]) + base).astype(BF16)

        toward = 1 - 2 * nd

        def z_copy(g, n, way, src, step):
            at = (halves[g], zcuts[g][n])
            return remote(
                src.at[at], zr.at[(way,) + at], z_ss.at[way], z_rs.at[way, place[g, n]], {"cand": j + step}
            )

        def z_wait(g, n, way):
            at = (halves[g], zcuts[g][n])
            remote(q_send.at[at], zr.at[(way,) + at], z_ss.at[way], z_rs.at[way, place[g, n]], {"cand": j}).wait_recv()

        def first_out(cols):
            last = cuts[n1 - 1]
            term = jnp.dot(cross1[:, last], w2_v[last, cols], preferred_element_type=F32)
            if n1 > 1:
                term = acc2[:, cols] + term
            owner = (j == i * ratio + cols.start // col).astype(F32)
            inside = cols.start % col
            carried = cross1[:, inside : inside + cols.stop - cols.start].astype(F32)
            term = base_mp[:, cols].astype(F32) * (term + owner * b2_ref[:, cols]) + owner * carried
            q_send[:, cols] = term.astype(BF16)

        for c in range(n1):
            first_cross(c)
            if c == 0:
                w2_copy.wait()
            if c < n1 - 1:
                with scope(f"l2_{c}"):
                    term = jnp.dot(cross1[:, cuts[c]], w2_v[cuts[c], :], preferred_element_type=F32)
                    acc2[...] = term if c == 0 else acc2[...] + term
            if c + ahead < n1:
                take_across(c + ahead)
        even = bit_of(0) == 0
        odd = jnp.logical_not(even)
        detour = jnp.logical_and(even, j == n_cand - 1) if n_cand > 2 else None

        def detour_copy(g, n):
            at = (halves[g], zcuts[g][n])
            return remote(
                q_send.at[at], ze.at[at], z_ss.at[1], ze_rs.at[place[g, n]], {"mp": i + 1, "cand": j - 1}
            )

        def first_send(g, ns):
            @pl.when(end if detour is None else jnp.logical_and(end, jnp.logical_not(detour)))
            def _():
                for n in ns:
                    z_copy(g, n, nd, q_send, toward).start()

            if detour is not None:
                @pl.when(detour)
                def _():
                    for n in ns:
                        detour_copy(g, n).start()

        def lend_copy(s):
            cols = slice(zcuts[0][s].start, zcuts[0][min(s + 1, len(zcuts[0]) - 1)].stop)
            return remote(q_send.at[:, cols], qe.at[:, cols], qe_ss.at[0], qe_rs.at[s // 2], {"mp": i + 1 - 2 * bit_of(0)})

        for s in range(0, len(zcuts[0]), 2):
            with scope(f"q{s}"):
                for cols in zcuts[0][s : s + 2]:
                    first_out(cols)
                first_send(0, range(s, min(s + 2, len(zcuts[0]))))

                @pl.when(jnp.logical_and(inner, even))
                def _():
                    lend_copy(s).start()

        for g in range(1, len(zcuts)):
            first_send(g, range(len(zcuts[g])))

        def pass_on(g, n, way, step):
            at = (halves[g], zcuts[g][n])
            zs[(way,) + at] = (zr[(way,) + at].astype(F32) + q_send[at].astype(F32)).astype(BF16)
            z_copy(g, n, way, zs.at[way], step).start()

        def near(g, n):
            with scope(f"near{g}_{n}"):
                z_wait(g, n, nd)
            pass_on(g, n, nd, toward)

        def far(g, n, passing):
            with scope(f"far{g}_{n}"):
                z_wait(g, n, 1 - nd)
            if passing:
                pass_on(g, n, 1 - nd, -toward)

        def relay(g, n):
            at = (halves[g], zcuts[g][n])
            k = place[g, n]
            with scope(f"relay{g}_{n}"):
                remote(ze.at[at], ze.at[at], ef_ss.at[0], ze_rs.at[k], {"cand": j}).wait_recv()
            if g == 0 and n % 2 == 0:
                lend_copy(n).wait_recv()
            zf[at] = (ze[at].astype(F32) + qe[at].astype(F32)).astype(BF16)

            @pl.when(j > 1)
            def _():
                remote(zf.at[at], ze.at[at], ef_ss.at[0], ze_rs.at[k], {"cand": j - 1}).start()

            @pl.when(j == 1)
            def _():
                remote(
                    zf.at[at], zr.at[(1,) + at], ef_ss.at[0], z_rs.at[1, k], {"mp": i - 1, "cand": j - 1}
                ).start()

            remote(ze.at[at], zr.at[(1,) + at], ef_ss.at[1], z_rs.at[1, k], {"mp": i - 1}).start()

        def third(g, n):
            cols = zcuts[g][n]
            r = halves[g]
            value = (
                q_send[r, cols].astype(F32) + zr[0, r, cols].astype(F32) + zr[1, r, cols].astype(F32)
            ).astype(BF16)
            x3[r, cols] = value
            if g == 0 and n == 0:
                w3_copy.wait()
            term = jnp.dot(value, w3_v[cols, :], preferred_element_type=F32)
            acc3[r, :] = term if n == 0 else acc3[r, :] + term

        def last_copy(c, peer):
            r = pl.ds(pl.multiple_of(peer * block, block), block)
            cols = slice(c * cw3, (c + 1) * cw3)
            return remote(send3.at[r, cols], recv3.at[i, :, cols], c_ss.at[0], c_rs.at[c], {"mp": peer})

        owner3 = (i == j // ratio).astype(F32)

        def q_copy(g, peer, dj):
            return remote(
                q_mine.at[g], q_all.at[me], q_sem.at[0], q_sem.at[1],
                {"mp": peer, "cand": lax.rem(j + dj, n_cand)},
            )

        def score_row(lanes, count):
            if q_width == 128:
                total = jnp.sum(lanes, axis=1, keepdims=True)
                row = lax.broadcasted_iota(jnp.int32, lanes.shape, 0)
                lane = lax.broadcasted_iota(jnp.int32, lanes.shape, 1)
                return jnp.sum(jnp.where(row == lane, total, 0.0), axis=0, keepdims=True)
            q_rows[0:count, :] = lanes
            return jnp.sum(q_rows[...].T, axis=0, keepdims=True)

        def epilogue(g):
            r = halves[g]
            for c in range(n3):
                cols = slice(c * cw3, (c + 1) * cw3)
                if ratio == 1:
                    carried = x3[r, cols]
                else:
                    carried = x3[r, pl.ds(pl.multiple_of(lax.rem(j, ratio) * col + c * cw3, 128), cw3)]
                term = (
                    base_col[r, cols].astype(F32) * (acc3[r, cols] + owner3 * b3_ref[:, cols])
                    + owner3 * carried.astype(F32)
                )
                acc3[r, cols] = term
                send3[r, cols] = term.astype(BF16)
            count = r.stop - r.start
            lanes = jnp.zeros((count, 128), F32)
            for k in range(0, col, 128):
                lanes = lanes + acc3[r, k : k + 128] * score_ref[k : k + 128].astype(F32).reshape(1, 128)
            q_mine[g] = score_row(lanes, count)

            def each(dj, carry):
                for peer in range(*spans[g]):
                    q_copy(g, peer, dj).start()
                return carry

            if n_cand <= 4:
                for dj in sorted(range(1, n_cand), key=lambda d: -min(d, n_cand - d)):
                    each(dj, 0)
            else:
                lax.fori_loop(1, n_cand, each, 0)
            for peer in range(*spans[g]):
                @pl.when(i != peer)
                def _():
                    q_copy(g, peer, 0).start()

                @pl.when(i == peer)
                def _():
                    q_all[me] = q_mine[g]

            for peer in range(*spans[g]):
                @pl.when(i != peer)
                def _():
                    for c in range(n3):
                        last_copy(c, peer).start()

        if q_width > 128:
            q_rows[...] = jnp.zeros(q_rows.shape, F32)

        def stream(skew, nears, passing, relays):
            ready_at = len(events) - skew if nears else 0
            lag = min(5, len(events)) if relays else 0
            for s in range(len(events) + skew + lag):
                if nears and s < len(events):
                    near(*events[s])
                back = s - lag if relays == 1 else s - skew - lag
                if relays == 1 and 0 <= back < len(events):
                    relay(*events[back])
                if 0 <= s - skew < len(events):
                    far(*events[s - skew], passing)
                if relays == 2 and 0 <= back < len(events):
                    relay(*events[back])
                if not 0 <= s - skew < len(events):
                    continue
                g, n = events[s - skew]
                if passing and not nears:
                    z_wait(g, n, nd)
                with scope(f"third{g}_{n}"):
                    third(g, n)
                for done in range(len(spans)):
                    last = place[done, len(zcuts[done]) - 1]
                    if s - skew == max(last, min(ready_at, len(events) - 1)):
                        with scope(f"epi{done}"):
                            epilogue(done)

        @pl.when(end)
        def _():
            stream(0, False, False, 0)

        if n_cand > 2:
            left = nd == 0

            @pl.when(jnp.logical_and(inner, jnp.logical_and(odd, left)))
            def _():
                stream(min(13, len(events)), True, True, 2)

            @pl.when(jnp.logical_and(inner, jnp.logical_and(odd, jnp.logical_not(left))))
            def _():
                stream(min(2, len(events)), True, True, 1)

            @pl.when(jnp.logical_and(inner, jnp.logical_and(even, left)))
            def _():
                stream(len(events), True, False, 0)

            @pl.when(jnp.logical_and(inner, jnp.logical_and(even, jnp.logical_not(left))))
            def _():
                stream(0, False, True, 0)

        mine = pl.ds(pl.multiple_of(i * block, block), block)
        for c in range(n3):
            cols = slice(c * cw3, (c + 1) * cw3)
            with scope(f"last{c}"):
                came = recv3.at[pl.ds(0, n_mp - 1), :, cols]
                remote(came, came, c_ss.at[0], c_rs.at[c], {"mp": i}).wait_recv()
            term = acc3[mine, cols]
            for d in range(1, n_mp):
                term = term + recv3[lax.rem(i - d + n_mp, n_mp), :, cols].astype(F32)
            out_ref[:, cols] = term.astype(BF16)

        with scope("qwait"):
            rest = q_all.at[pl.ds(0, group - 1)]
            remote(rest, rest, q_sem.at[0], q_sem.at[1], {"cand": j}).wait_recv()
            total = jnp.sum(q_all[...], axis=0)
            for lo, hi in spans:
                for k in range(lo, hi):
                    @pl.when(i == k)
                    def _():
                        logit_ref[...] = total[:, (k - lo) * block : (k - lo + 1) * block]

        def sent(ref, sem):
            remote(ref, ref, sem, sem, {"cand": j}).wait_send()

        with scope("sent"):
            for b in range(low):
                @pl.when(jnp.logical_and(pool_side, jnp.logical_and(ones(b), bit_of(b) == 0)))
                def _():
                    sent(send1, a_ss.at[b])

                @pl.when(ones(b + 1))
                def _():
                    sent(psum, g_ss.at[b])

            @pl.when(jnp.logical_and(pool_side, root))
            def _():
                sent(psum, x_ss.at[0])

            @pl.when(user_side)
            def _():
                @pl.when(leader)
                def _():
                    sent(others, user_sem.at[0])
                    for d in range(1, half):
                        sent(urow, urow_ss.at[d])

                @pl.when(jnp.logical_not(col_pool))
                def _():
                    sent(ucol, ucol_sem.at[0])

                sent(ubuf.at[pl.ds(0, n_mp - 1)], u_ss.at[0])

            @pl.when(end)
            def _():
                sent(q_send, z_ss.at[nd])

            @pl.when(inner)
            def _():
                sent(q_send, z_ss.at[0])

            @pl.when(jnp.logical_and(inner, odd))
            def _():
                for sem in (z_ss.at[1], ef_ss.at[0], ef_ss.at[1]):
                    sent(q_send, sem)

            @pl.when(jnp.logical_and(inner, even))
            def _():
                sent(q_send, qe_ss.at[0])

            sent(recv3.at[pl.ds(0, n_mp - 1)], c_ss.at[0])
            sent(rest, q_sem.at[0])

    return kernel


def solution(mesh):
    n_mp, n_cand = mesh.shape["mp"], mesh.shape["cand"]

    def body(
        user_feats, user_slot, cand_pool, cand_ids, first_weight, first_bias,
        second_weight, second_bias, third_weight, third_bias, score_weight,
    ):
        slots_each, half_width = user_feats.shape
        users, per_user = cand_ids.shape
        rows = users * per_user
        pool_count = cand_pool.shape[0]
        feat, col = first_weight.shape
        wide = min(512, col)
        ucuts = [slice(k, k + wide) for k in range(0, col, wide)]
        cuts = list(ucuts)
        half = n_mp // 2
        spans = [(0, half), (half, n_mp)]
        zcuts = []
        for lo, hi in spans:
            step = min(256 * half // (hi - lo), col, feat)
            zcuts.append([slice(k, k + step) for k in range(0, feat, step)])
        if step > 128:
            zcuts[-1][-1:] = [slice(feat - step, feat - step // 2), slice(feat - step // 2, feat)]
        n1 = len(cuts)
        n3 = max(1, col // 512)
        lhs_rows = -(-users // 16) * 16
        bits = n_mp.bit_length() - 1
        low = max(1, bits - 1)
        block = rows // n_mp
        group = n_mp * n_cand
        shapes = (rows, per_user, users, slots_each, half_width, pool_count, feat, col, cuts, ucuts, zcuts, spans, n3)
        vmem = pl.BlockSpec(memory_space=pltpu.VMEM)
        hbm = pl.BlockSpec(memory_space=pl.ANY)
        dma = pltpu.SemaphoreType.DMA
        crossed, logits = pl.pallas_call(
            make_kernel(n_mp, n_cand, shapes),
            out_shape=(
                pltpu.VMEM((block, col), BF16),
                pltpu.VMEM((1, block), F32),
            ),
            in_specs=[hbm] * 11,
            out_specs=(vmem, vmem),
            scratch_shapes=[
                pltpu.SMEM((1, users), jnp.int32),
                pltpu.VMEM((users, per_user), jnp.int32),
                pltpu.VMEM((1, col), F32),
                pltpu.VMEM((1, feat), F32),
                pltpu.VMEM((1, col), F32),
                pltpu.VMEM((col,), BF16),
                dma((7,)),
                pltpu.VMEM((n_cand, slots_each, half_width), BF16),
                pltpu.VMEM((users, half_width), BF16),
                pltpu.VMEM((users, col), BF16),
                pltpu.VMEM((pool_count, feat), BF16),
                pltpu.VMEM((pool_count, col), BF16),
                pltpu.VMEM((feat, col), BF16),
                pltpu.VMEM((col, feat), BF16),
                pltpu.VMEM((feat, col), BF16),
                pltpu.VMEM((rows, pool_count), BF16),
                pltpu.VMEM((rows, feat), BF16),
                pltpu.VMEM((rows, col), BF16),
                pltpu.VMEM((lhs_rows, feat), BF16),
                pltpu.VMEM((rows, col), F32),
                pltpu.VMEM((rows, col), BF16),
                pltpu.VMEM((low, rows, col), BF16),
                pltpu.VMEM((rows, col), BF16),
                pltpu.VMEM((n_mp, users, col), F32),
                pltpu.VMEM((rows, col), BF16),
                pltpu.VMEM((rows, feat), F32),
                pltpu.VMEM((rows, feat), BF16),
                pltpu.VMEM((2, rows, feat), BF16),
                pltpu.VMEM((2, rows, feat), BF16),
                pltpu.VMEM((rows, feat), BF16),
                pltpu.VMEM((rows, feat), BF16),
                pltpu.VMEM((rows, feat), BF16),
                pltpu.VMEM((rows, feat), BF16),
                pltpu.VMEM((rows, col), F32),
                pltpu.VMEM((rows, col), BF16),
                pltpu.VMEM((n_mp, block, col), BF16),
                pltpu.VMEM((max(rows // 2, 128), 128), F32),
                pltpu.VMEM((len(spans), 1, max(rows // 2, 128)), F32),
                pltpu.VMEM((group, 1, max(rows // 2, 128)), F32),
                dma((4 + n1,)),
                dma((2,)),
                dma((half,)),
                dma((1,)),
                dma((2,)),
                pltpu.SemaphoreType.REGULAR((1,)),
                dma((low,)),
                dma((low, n1)),
                dma((1,)),
                dma((n1,)),
                dma((low,)),
                dma((n1,)),
                dma((1,)),
                dma((len(ucuts),)),
                dma((2,)),
                dma((2, sum(len(part) for part in zcuts))),
                dma((sum(len(part) for part in zcuts),)),
                dma((1,)),
                dma((-(-len(zcuts[0]) // 2),)),
                dma((2,)),
                dma((1,)),
                dma((n3,)),
                dma((2,)),
            ],
            compiler_params=pltpu.CompilerParams(
                collective_id=0, has_side_effects=True, vmem_limit_bytes=67043328 - 3000 * 1024
            ),
        )(
            user_feats, user_slot.reshape(1, -1), cand_pool, cand_ids, first_weight, first_bias.reshape(1, -1),
            second_weight, second_bias.reshape(1, -1), third_weight, third_bias.reshape(1, -1),
            score_weight,
        )
        crossed, logits = pl.pallas_call(
            hand_on,
            out_shape=(
                jax.ShapeDtypeStruct((block, col), BF16),
                jax.ShapeDtypeStruct((1, block), F32),
            ),
            in_specs=[vmem, vmem],
            out_specs=(hbm, hbm),
            scratch_shapes=[dma((2,))],
            compiler_params=pltpu.CompilerParams(vmem_limit_bytes=1024 * 1024),
        )(crossed, logits)
        return crossed, logits.reshape(-1)

    in_specs = (
        P(("groups", "cand"), None),
        P("groups"),
        P("groups", None),
        P("groups", None),
        P("mp", "cand"),
        P("cand"),
        P("cand", "mp"),
        P("mp"),
        P("mp", "cand"),
        P("cand"),
        P("cand"),
    )
    out_specs = (P(("groups", "mp"), "cand"), P(("groups", "mp")))
    return jax.shard_map(body, mesh=mesh, in_specs=in_specs, out_specs=out_specs, check_vma=False)
```

```python
import contextlib

import jax
import jax.numpy as jnp
from jax import lax
from jax.experimental import pallas as pl
from jax.experimental.pallas import tpu as pltpu
from jax.sharding import PartitionSpec as P

MESH = pl.DeviceIdType.MESH
F32 = jnp.float32
BF16 = jnp.bfloat16


def scope(name):
    return contextlib.nullcontext()


def hand_on(crossed_ref, logit_ref, crossed_hbm, logit_hbm, sem):
    copies = [
        pltpu.make_async_copy(crossed_ref, crossed_hbm, sem.at[0]),
        pltpu.make_async_copy(logit_ref, logit_hbm, sem.at[1]),
    ]
    for copy in copies:
        copy.start()
    for copy in copies:
        copy.wait()


def make_kernel(n_mp, n_cand, shapes):
    rows, per_user, users, slots_each, half_width, pool_count, feat, col, cuts, ucuts, zcuts, spans, n3 = shapes
    cw3 = col // n3
    n1 = len(cuts)
    bits = n_mp.bit_length() - 1
    low = bits - 1
    half = n_mp // 2
    block = rows // n_mp
    ratio = feat // col
    group = n_mp * n_cand
    halves = [slice(lo * block, hi * block) for lo, hi in spans]
    events = [(g, n) for g in range(len(spans)) for n in range(len(zcuts[g]))]
    place = {event: k for k, event in enumerate(events)}
    q_width = max([128] + [r.stop - r.start for r in halves])
    first_pool_col = half_width // col

    def user_of(p):
        return (p * block) // per_user

    def kernel(
        user_hbm, slot_hbm, pool_hbm, ids_hbm, w1_hbm, b1_hbm, w2_hbm, b2_hbm, w3_hbm, b3_hbm, score_hbm,
        out_ref, logit_ref,
        slot_ref, ids_ref, b1_ref, b2_ref, b3_ref, score_ref, small_sem, slots, urow, ucol, pool_m, pool_c, w1_v, w2_v, w3_v,
        onehot, base_mp, base_col, lhs, acc1, send1, recv1, psum, ubuf, cross1, acc2, q_send, zr, zs, ze, zf, qe, x3, acc3, send3, recv3,
        q_rows, q_mine, q_all,
        w_sem, user_sem, urow_ss, urow_rs, ucol_sem, ready, a_ss, a_rs, x_ss, x_rs, g_ss, g_rs, u_ss, u_rs, z_ss, z_rs, ze_rs, qe_ss, qe_rs, ef_ss, c_ss, c_rs, q_sem,
    ):
        i = lax.axis_index("mp")
        j = lax.axis_index("cand")
        me = i * n_cand + j
        user_side = i < half
        pool_side = jnp.logical_not(user_side)
        leader = i == half - 1
        follower = jnp.logical_not(leader)

        def remote(src, dst, ss, rs, where):
            return pltpu.make_async_remote_copy(
                src_ref=src, dst_ref=dst, send_sem=ss, recv_sem=rs, device_id=where, device_id_type=MESH
            )

        barrier = pltpu.get_barrier_semaphore()
        with scope("greet"):
            def greet(d, carry):
                pl.semaphore_signal(barrier, inc=1, device_id={"cand": lax.rem(j + d, n_cand)}, device_id_type=MESH)
                return carry

            @pl.when(leader)
            def _():
                lax.fori_loop(1, n_cand, greet, 0, unroll=n_cand <= 4)

            @pl.when(jnp.logical_and(follower, j > 0))
            def _():
                pl.semaphore_signal(barrier, inc=1, device_id={"cand": j - 1}, device_id_type=MESH)

            @pl.when(jnp.logical_and(follower, j < n_cand - 1))
            def _():
                pl.semaphore_signal(barrier, inc=1, device_id={"cand": j + 1}, device_id_type=MESH)

            @pl.when(user_side)
            def _():
                for d in range(1, n_mp):
                    pl.semaphore_signal(barrier, inc=1, device_id={"mp": lax.rem(i + d, n_mp)}, device_id_type=MESH)

            @pl.when(pool_side)
            def _():
                for d in range(1, half):
                    pl.semaphore_signal(
                        barrier, inc=1, device_id={"mp": half + lax.rem(i + d, half)}, device_id_type=MESH
                    )

        small_copies = [
            pltpu.make_async_copy(src, dst, small_sem.at[k])
            for k, (src, dst) in enumerate(
                (
                    (ids_hbm, ids_ref), (slot_hbm, slot_ref), (user_hbm, slots.at[j]), (b1_hbm, b1_ref),
                    (b2_hbm, b2_ref), (b3_hbm, b3_ref), (score_hbm, score_ref),
                )
            )
        ]
        m_start = pl.multiple_of(jnp.maximum(i - half, 0) * feat, 128)
        c_start = pl.multiple_of(jnp.maximum(j - first_pool_col, 0) * col, 128)
        pool_m_copy = pltpu.make_async_copy(pool_hbm.at[:, pl.ds(m_start, feat)], pool_m, w_sem.at[0])
        pool_c_copy = pltpu.make_async_copy(pool_hbm.at[:, pl.ds(c_start, col)], pool_c, w_sem.at[1])
        w1_copies = [
            pltpu.make_async_copy(w1_hbm.at[:, cut], w1_v.at[:, cut], w_sem.at[2 + c]) for c, cut in enumerate(cuts)
        ]
        w2_copy = pltpu.make_async_copy(w2_hbm, w2_v, w_sem.at[2 + n1])
        w3_copy = pltpu.make_async_copy(w3_hbm, w3_v, w_sem.at[3 + n1])
        col_pool = j >= first_pool_col
        with scope("loads"):
            for copy in small_copies[:3]:
                copy.start()

            @pl.when(pool_side)
            def _():
                pool_m_copy.start()

            for copy in w1_copies:
                copy.start()
            for copy in small_copies[3:]:
                copy.start()

            @pl.when(col_pool)
            def _():
                pool_c_copy.start()

            @pl.when(user_side)
            def _():
                w2_copy.start()

            end = jnp.logical_or(j == 0, j == n_cand - 1)
            inner = jnp.logical_not(end)
            nd = (j >= (n_cand + 1) // 2).astype(jnp.int32)

            @pl.when(end)
            def _():
                zr[nd] = jnp.zeros(zr.shape[1:], BF16)

        def build_onehot():
            with scope("onehot"):
                small_copies[0].wait()
                for u in range(users):
                    hot = (
                        lax.broadcasted_iota(jnp.int32, (pool_count, per_user), 0) == ids_ref[u : u + 1, :]
                    ).astype(F32).T
                    for p in range(n_mp):
                        first = p * block
                        if first // per_user == u:
                            off = first % per_user
                            onehot[p * block : (p + 1) * block, :] = hot[off : off + block].astype(BF16)

        def from_pool(dst, src, width):
            for c in range(0, width, 256):
                dst[:, c : c + 256] = jnp.dot(onehot[...], src[:, c : c + 256], preferred_element_type=F32).astype(BF16)

        def user_row(u):
            slot = slot_ref[0, u]
            row = slots[slot // slots_each].astype(F32)
            if slots_each > 1:
                pick = lax.broadcasted_iota(jnp.int32, row.shape, 0) == lax.rem(slot, slots_each)
                row = jnp.sum(jnp.where(pick, row, 0.0), axis=0, keepdims=True)
            return row

        def from_user(dst, index, width):
            row = urow[:, pl.ds(pl.multiple_of(index * width, 128), width)].astype(F32)
            for p in range(n_mp):
                u = user_of(p)
                dst[p * block : (p + 1) * block, :] = jnp.broadcast_to(row[u : u + 1], (block, width)).astype(BF16)

        def urow_copy(d):
            return remote(urow, urow, urow_ss.at[d], urow_rs.at[0], {"mp": lax.rem(i + d, half)})

        def user_copy(k):
            d = jnp.where(j < n_cand // 2, n_cand - k, k)
            return remote(user_hbm, slots.at[j], user_sem.at[0], user_sem.at[1], {"cand": lax.rem(j + d, n_cand)})

        def ucol_copy():
            return remote(ucol, ucol, ucol_sem.at[0], ucol_sem.at[1], {"mp": lax.rem(i + half, n_mp)})

        others = slots.at[pl.ds(0, n_cand - 1)]

        def from_all_users():
            remote(others, others, user_sem.at[0], user_sem.at[1], {"cand": j}).wait_recv()
            small_copies[1].wait()

        def bit_of(b):
            return lax.rem(i // (1 << b), 2)

        def partner(b):
            return i + (1 << b) * (1 - 2 * bit_of(b))

        def ones(b):
            return lax.rem(i, 1 << b) == (1 << b) - 1

        root = ones(low)
        leaf = jnp.logical_not(root)

        def tree_copy(c, b):
            return remote(
                send1.at[:, cuts[c]], recv1.at[b, :, cuts[c]], a_ss.at[b], a_rs.at[b, c], {"mp": partner(b)}
            )

        def across_copy(c):
            return remote(
                psum.at[:, cuts[c]], psum.at[:, cuts[c]], x_ss.at[0], x_rs.at[c], {"mp": lax.rem(i + half, n_mp)}
            )

        def spread_copy(c, b):
            return remote(psum.at[:, cuts[c]], psum.at[:, cuts[c]], g_ss.at[b], g_rs.at[c], {"mp": partner(b)})

        def reduce(c, b):
            cut = cuts[c]
            if b == low:
                psum[:, cut] = acc1[:, cut].astype(BF16)
                hand_out(c)
                return

            @pl.when(bit_of(b) == 0)
            def _():
                send1[:, cut] = acc1[:, cut].astype(BF16)
                tree_copy(c, b).start()

            @pl.when(bit_of(b) != 0)
            def _():
                tree_copy(c, b).wait_recv()
                acc1[:, cut] = acc1[:, cut] + recv1[b, :, cut].astype(F32)
                reduce(c, b + 1)

        def hand_out(c):
            across_copy(c).start()
            for b in range(low - 1, -1, -1):
                spread_copy(c, b).start()

        def stage_a(c, sends):
            w1_copies[c].wait()
            term = jnp.dot(base_mp[...], w1_v[:, cuts[c]], preferred_element_type=F32)
            if sends:
                send1[:, cuts[c]] = term.astype(BF16)
                tree_copy(c, 0).start()
            else:
                acc1[:, cuts[c]] = term

        def stage_b(c):
            if low == 1:
                cut = cuts[c]
                tree_copy(c, 0).wait_recv()
                psum[:, cut] = (acc1[:, cut] + recv1[0, :, cut].astype(F32)).astype(BF16)
                hand_out(c)
            else:
                reduce(c, 0)

        def part_copy(c, d):
            return remote(ubuf.at[i, :, ucuts[c]], ubuf.at[i, :, ucuts[c]], u_ss.at[0], u_rs.at[c], {"mp": lax.rem(i + d, n_mp)})

        def part_wait(c, count):
            came = ubuf.at[pl.ds(0, count), :, ucuts[c]]
            remote(came, came, u_ss.at[0], u_rs.at[c], {"cand": j}).wait_recv()

        with scope("firstpart"):
            @pl.when(pool_side)
            def _():
                build_onehot()
                pool_m_copy.wait()
                from_pool(base_mp, pool_m, feat)

        neighbours = (j > 0).astype(jnp.int32) + (j < n_cand - 1).astype(jnp.int32)
        with scope("barrier"):
            pl.semaphore_wait(
                barrier,
                jnp.where(leader, n_cand - 1, neighbours) + jnp.where(user_side, half - 1, n_mp - 1),
            )

        with scope("layer1"):
            @pl.when(pool_side)
            def _():
                for d in range(half):
                    pl.semaphore_signal(ready.at[0], inc=1, device_id={"mp": d}, device_id_type=MESH)
                def pool_part(sends):
                    lag = n1 if sends else 2
                    for c in range(n1 + lag):
                        if c < n1:
                            with scope(f"a{c}"):
                                stage_a(c, sends)
                            if c == n1 - 1:
                                w2_copy.start()
                        if c >= lag and not sends:
                            with scope(f"b{c - lag}"):
                                stage_b(c - lag)

                if low > 0:
                    @pl.when(bit_of(0) == 0)
                    def _():
                        pool_part(True)

                    @pl.when(bit_of(0) != 0)
                    def _():
                        pool_part(False)
                else:
                    pool_part(False)

            @pl.when(user_side)
            def _():
                @pl.when(leader)
                def _():
                    for k in range(1, n_cand):
                        user_copy(k).start()

                with scope("early"):
                    @pl.when(col_pool)
                    def _():
                        build_onehot()
                        pool_c_copy.wait()
                        from_pool(base_col, pool_c, col)

                    @pl.when(jnp.logical_not(col_pool))
                    def _():
                        small_copies[0].wait()

                    for copy in w1_copies:
                        copy.wait()
                    small_copies[2].wait()
                    pl.semaphore_wait(ready.at[0], half)
                with scope("users"):
                    @pl.when(leader)
                    def _():
                        from_all_users()
                        for u in range(users):
                            urow[u : u + 1, :] = user_row(u).astype(BF16)
                        for d in range(1, half):
                            urow_copy(d).start()

                    @pl.when(follower)
                    def _():
                        if half > 1:
                            urow_copy(0).wait_recv()
                        small_copies[1].wait()

                row = urow[:, pl.ds(pl.multiple_of(i * feat, 128), feat)]
                if users == 1:
                    lhs[...] = jnp.broadcast_to(row.astype(F32), lhs.shape).astype(BF16)
                else:
                    line = lax.broadcasted_iota(jnp.int32, lhs.shape, 0)
                    filled = jnp.zeros(lhs.shape, F32)
                    for u in range(users):
                        filled = jnp.where(line == u, row[u : u + 1].astype(F32), filled)
                    lhs[...] = filled.astype(BF16)
                for c, cut in enumerate(ucuts):
                    with scope(f"um{c}"):
                        term = jnp.dot(lhs[...], w1_v[:, cut], preferred_element_type=F32)
                        ubuf[i, :, cut] = term[0:users]
                        for d in range(n_mp - 1, 0, -1):
                            part_copy(c, d).start()
                    if c == 0:
                        @pl.when(jnp.logical_not(col_pool))
                        def _():
                            ucol[...] = urow[:, pl.ds(pl.multiple_of(j * col, 128), col)]
                            ucol_copy().start()

        def take_across(c):
            @pl.when(jnp.logical_and(user_side, root))
            def _():
                with scope(f"across{c}"):
                    across_copy(c).wait_recv()
                for b in range(low - 1, -1, -1):
                    spread_copy(c, b).start()

        ahead = 1
        with scope("bases"):
            w3_copy.start()

            for c in range(ahead):
                take_across(c)

            @pl.when(user_side)
            def _():
                from_user(base_mp, i, feat)

            @pl.when(jnp.logical_and(col_pool, pool_side))
            def _():
                pool_c_copy.wait()
                from_pool(base_col, pool_c, col)

            @pl.when(jnp.logical_not(col_pool))
            def _():
                @pl.when(pool_side)
                def _():
                    ucol_copy().wait_recv()

                for p in range(n_mp):
                    u = user_of(p)
                    value = ucol[u : u + 1, :].astype(F32)
                    base_col[p * block : (p + 1) * block, :] = jnp.broadcast_to(value, (block, col)).astype(BF16)

            for copy in small_copies[3:]:
                copy.wait()

            @pl.when(pool_side)
            def _():
                for copy in small_copies[1:3]:
                    copy.wait()

        def first_cross(c):
            if low > 0:
                @pl.when(leaf)
                def _():
                    with scope(f"gw{c}"):
                        spread_copy(c, 0).wait_recv()

                for b in range(low - 2, -1, -1):
                    @pl.when(jnp.logical_and(leaf, ones(b + 1)))
                    def _():
                        spread_copy(c, b).start()

            for u, ucut in enumerate(ucuts):
                if ucut.start != cuts[c].start:
                    continue
                with scope(f"pw{u}"):
                    @pl.when(user_side)
                    def _():
                        if half > 1:
                            part_wait(u, half - 1)

                    @pl.when(pool_side)
                    def _():
                        part_wait(u, half)

            cols = cuts[c]
            added = b1_ref[:, cols]
            for src in range(half):
                added = added + ubuf[src, :, cols]
            for p in range(n_mp):
                r = slice(p * block, (p + 1) * block)
                u = user_of(p)
                base = base_col[r, cols].astype(F32)
                cross1[r, cols] = (base * (psum[r, cols].astype(F32) + added[u : u + 1]) + base).astype(BF16)

        toward = 1 - 2 * nd

        def z_copy(g, n, way, src, step):
            at = (halves[g], zcuts[g][n])
            return remote(
                src.at[at], zr.at[(way,) + at], z_ss.at[way], z_rs.at[way, place[g, n]], {"cand": j + step}
            )

        def z_wait(g, n, way):
            at = (halves[g], zcuts[g][n])
            remote(q_send.at[at], zr.at[(way,) + at], z_ss.at[way], z_rs.at[way, place[g, n]], {"cand": j}).wait_recv()

        def first_out(cols):
            last = cuts[n1 - 1]
            term = jnp.dot(cross1[:, last], w2_v[last, cols], preferred_element_type=F32)
            if n1 > 1:
                term = acc2[:, cols] + term
            owner = (j == i * ratio + cols.start // col).astype(F32)
            inside = cols.start % col
            carried = cross1[:, inside : inside + cols.stop - cols.start].astype(F32)
            term = base_mp[:, cols].astype(F32) * (term + owner * b2_ref[:, cols]) + owner * carried
            q_send[:, cols] = term.astype(BF16)

        for c in range(n1):
            first_cross(c)
            if c == 0:
                w2_copy.wait()
            if c < n1 - 1:
                with scope(f"l2_{c}"):
                    term = jnp.dot(cross1[:, cuts[c]], w2_v[cuts[c], :], preferred_element_type=F32)
                    acc2[...] = term if c == 0 else acc2[...] + term
            if c + ahead < n1:
                take_across(c + ahead)
        even = bit_of(0) == 0
        odd = jnp.logical_not(even)
        detour = jnp.logical_and(even, j == n_cand - 1) if n_cand > 2 else None

        def detour_copy(g, n):
            at = (halves[g], zcuts[g][n])
            return remote(
                q_send.at[at], ze.at[at], z_ss.at[1], ze_rs.at[place[g, n]], {"mp": i + 1, "cand": j - 1}
            )

        def first_send(g, ns):
            @pl.when(end if detour is None else jnp.logical_and(end, jnp.logical_not(detour)))
            def _():
                for n in ns:
                    z_copy(g, n, nd, q_send, toward).start()

            if detour is not None:
                @pl.when(detour)
                def _():
                    for n in ns:
                        detour_copy(g, n).start()

        def lend_copy(s):
            cols = slice(zcuts[0][s].start, zcuts[0][min(s + 1, len(zcuts[0]) - 1)].stop)
            return remote(q_send.at[:, cols], qe.at[:, cols], qe_ss.at[0], qe_rs.at[0], {"mp": i + 1 - 2 * bit_of(0)})

        for s in range(0, len(zcuts[0]), 2):
            with scope(f"q{s}"):
                if s == 0:
                    for n in range(min(2, len(zcuts[0]))):
                        first_out(zcuts[0][n])
                        first_send(0, [n])
                else:
                    for cols in zcuts[0][s : s + 2]:
                        first_out(cols)
                    first_send(0, range(s, min(s + 2, len(zcuts[0]))))

                @pl.when(jnp.logical_and(inner, even))
                def _():
                    lend_copy(s).start()

        for g in range(1, len(zcuts)):
            first_send(g, range(len(zcuts[g])))

        def pass_on(g, n, way, step):
            at = (halves[g], zcuts[g][n])
            zs[(way,) + at] = (zr[(way,) + at].astype(F32) + q_send[at].astype(F32)).astype(BF16)
            z_copy(g, n, way, zs.at[way], step).start()

        def near(g, n):
            with scope(f"near{g}_{n}"):
                z_wait(g, n, nd)
            pass_on(g, n, nd, toward)

        def far(g, n, passing):
            with scope(f"far{g}_{n}"):
                z_wait(g, n, 1 - nd)
            if passing:
                pass_on(g, n, 1 - nd, -toward)

        def relay(g, n):
            at = (halves[g], zcuts[g][n])
            k = place[g, n]
            with scope(f"relay{g}_{n}"):
                remote(ze.at[at], ze.at[at], ef_ss.at[0], ze_rs.at[k], {"cand": j}).wait_recv()
            if k == 0:
                remote(q_send, qe, qe_ss.at[0], qe_rs.at[0], {"cand": j}).wait_recv()
            zf[at] = (ze[at].astype(F32) + qe[at].astype(F32)).astype(BF16)

            @pl.when(j > 1)
            def _():
                remote(zf.at[at], ze.at[at], ef_ss.at[0], ze_rs.at[k], {"cand": j - 1}).start()

            @pl.when(j == 1)
            def _():
                remote(
                    zf.at[at], zr.at[(1,) + at], ef_ss.at[0], z_rs.at[1, k], {"mp": i - 1, "cand": j - 1}
                ).start()

            remote(ze.at[at], zr.at[(1,) + at], ef_ss.at[1], z_rs.at[1, k], {"mp": i - 1}).start()

        def third(g, n):
            cols = zcuts[g][n]
            r = halves[g]
            value = (
                q_send[r, cols].astype(F32) + zr[0, r, cols].astype(F32) + zr[1, r, cols].astype(F32)
            ).astype(BF16)
            x3[r, cols] = value
            if g == 0 and n == 0:
                w3_copy.wait()
            term = jnp.dot(value, w3_v[cols, :], preferred_element_type=F32)
            acc3[r, :] = term if n == 0 else acc3[r, :] + term

        def last_copy(c, peer):
            r = pl.ds(pl.multiple_of(peer * block, block), block)
            cols = slice(c * cw3, (c + 1) * cw3)
            return remote(send3.at[r, cols], recv3.at[i, :, cols], c_ss.at[0], c_rs.at[c], {"mp": peer})

        owner3 = (i == j // ratio).astype(F32)

        def q_copy(g, peer, dj):
            return remote(
                q_mine.at[g], q_all.at[me], q_sem.at[0], q_sem.at[1],
                {"mp": peer, "cand": lax.rem(j + dj, n_cand)},
            )

        def score_row(lanes, count):
            if q_width == 128:
                total = jnp.sum(lanes, axis=1, keepdims=True)
                row = lax.broadcasted_iota(jnp.int32, lanes.shape, 0)
                lane = lax.broadcasted_iota(jnp.int32, lanes.shape, 1)
                return jnp.sum(jnp.where(row == lane, total, 0.0), axis=0, keepdims=True)
            q_rows[0:count, :] = lanes
            return jnp.sum(q_rows[...].T, axis=0, keepdims=True)

        def epilogue(g):
            r = halves[g]
            for c in range(n3):
                cols = slice(c * cw3, (c + 1) * cw3)
                if ratio == 1:
                    carried = x3[r, cols]
                else:
                    carried = x3[r, pl.ds(pl.multiple_of(lax.rem(j, ratio) * col + c * cw3, 128), cw3)]
                term = (
                    base_col[r, cols].astype(F32) * (acc3[r, cols] + owner3 * b3_ref[:, cols])
                    + owner3 * carried.astype(F32)
                )
                acc3[r, cols] = term
                send3[r, cols] = term.astype(BF16)
            def send_parts(lo, hi):
                for peer in range(lo, hi):
                    @pl.when(i != peer)
                    def _():
                        for c in range(n3):
                            last_copy(c, peer).start()

            send_parts(spans[g][0], spans[g][0] + 1)
            count = r.stop - r.start
            lanes = jnp.zeros((count, 128), F32)
            for k in range(0, col, 128):
                lanes = lanes + acc3[r, k : k + 128] * score_ref[k : k + 128].astype(F32).reshape(1, 128)
            q_mine[g] = score_row(lanes, count)

            def each(dj, carry):
                for peer in range(*spans[g]):
                    q_copy(g, peer, dj).start()
                return carry

            if n_cand <= 4:
                for dj in sorted(range(1, n_cand), key=lambda d: -min(d, n_cand - d)):
                    each(dj, 0)
            else:
                lax.fori_loop(1, n_cand, each, 0)
            for peer in range(*spans[g]):
                @pl.when(i != peer)
                def _():
                    q_copy(g, peer, 0).start()

                @pl.when(i == peer)
                def _():
                    q_all[me] = q_mine[g]

            send_parts(spans[g][0] + 1, spans[g][1])

        if q_width > 128:
            q_rows[...] = jnp.zeros(q_rows.shape, F32)

        def stream(skew, nears, passing, relays):
            ready_at = len(events) - skew if nears else 0
            lag = min(5, len(events)) if relays else 0
            for s in range(len(events) + skew + lag):
                if nears and s < len(events):
                    near(*events[s])
                back = s - lag if relays == 1 else s - skew - lag
                if relays == 1 and 0 <= back < len(events):
                    relay(*events[back])
                if 0 <= s - skew < len(events):
                    far(*events[s - skew], passing)
                if relays == 2 and 0 <= back < len(events):
                    relay(*events[back])
                if not 0 <= s - skew < len(events):
                    continue
                g, n = events[s - skew]
                if passing and not nears:
                    z_wait(g, n, nd)
                with scope(f"third{g}_{n}"):
                    third(g, n)
                for done in range(len(spans)):
                    last = place[done, len(zcuts[done]) - 1]
                    if s - skew == max(last, min(ready_at, len(events) - 1)):
                        with scope(f"epi{done}"):
                            epilogue(done)

        @pl.when(end)
        def _():
            stream(0, False, False, 0)

        if n_cand > 2:
            left = nd == 0

            @pl.when(jnp.logical_and(inner, jnp.logical_and(odd, left)))
            def _():
                stream(min(13, len(events)), True, True, 2)

            @pl.when(jnp.logical_and(inner, jnp.logical_and(odd, jnp.logical_not(left))))
            def _():
                stream(min(2, len(events)), True, True, 1)

            @pl.when(jnp.logical_and(inner, jnp.logical_and(even, left)))
            def _():
                stream(len(events), True, False, 0)

            @pl.when(jnp.logical_and(inner, jnp.logical_and(even, jnp.logical_not(left))))
            def _():
                stream(0, False, True, 0)

        mine = pl.ds(pl.multiple_of(i * block, block), block)
        for c in range(n3):
            cols = slice(c * cw3, (c + 1) * cw3)
            with scope(f"last{c}"):
                came = recv3.at[pl.ds(0, n_mp - 1), :, cols]
                remote(came, came, c_ss.at[0], c_rs.at[c], {"mp": i}).wait_recv()
            term = acc3[mine, cols]
            for d in range(1, n_mp):
                term = term + recv3[lax.rem(i - d + n_mp, n_mp), :, cols].astype(F32)
            out_ref[:, cols] = term.astype(BF16)

        with scope("qwait"):
            rest = q_all.at[pl.ds(0, group - 1)]
            remote(rest, rest, q_sem.at[0], q_sem.at[1], {"cand": j}).wait_recv()
            total = jnp.sum(q_all[...], axis=0)
            for lo, hi in spans:
                for k in range(lo, hi):
                    @pl.when(i == k)
                    def _():
                        logit_ref[...] = total[:, (k - lo) * block : (k - lo + 1) * block]

        def sent(ref, sem):
            remote(ref, ref, sem, sem, {"cand": j}).wait_send()

        with scope("sent"):
            for b in range(low):
                @pl.when(jnp.logical_and(pool_side, jnp.logical_and(ones(b), bit_of(b) == 0)))
                def _():
                    sent(send1, a_ss.at[b])

                @pl.when(ones(b + 1))
                def _():
                    sent(psum, g_ss.at[b])

            @pl.when(jnp.logical_and(pool_side, root))
            def _():
                sent(psum, x_ss.at[0])

            @pl.when(user_side)
            def _():
                @pl.when(leader)
                def _():
                    sent(others, user_sem.at[0])
                    for d in range(1, half):
                        sent(urow, urow_ss.at[d])

                @pl.when(jnp.logical_not(col_pool))
                def _():
                    sent(ucol, ucol_sem.at[0])

                sent(ubuf.at[pl.ds(0, n_mp - 1)], u_ss.at[0])

            @pl.when(end)
            def _():
                sent(q_send, z_ss.at[nd])

            @pl.when(inner)
            def _():
                sent(q_send, z_ss.at[0])

            @pl.when(jnp.logical_and(inner, odd))
            def _():
                for sem in (z_ss.at[1], ef_ss.at[0], ef_ss.at[1]):
                    sent(q_send, sem)

            @pl.when(jnp.logical_and(inner, even))
            def _():
                sent(q_send, qe_ss.at[0])

            sent(recv3.at[pl.ds(0, n_mp - 1)], c_ss.at[0])
            sent(rest, q_sem.at[0])

    return kernel


def solution(mesh):
    n_mp, n_cand = mesh.shape["mp"], mesh.shape["cand"]

    def body(
        user_feats, user_slot, cand_pool, cand_ids, first_weight, first_bias,
        second_weight, second_bias, third_weight, third_bias, score_weight,
    ):
        slots_each, half_width = user_feats.shape
        users, per_user = cand_ids.shape
        rows = users * per_user
        pool_count = cand_pool.shape[0]
        feat, col = first_weight.shape
        wide = min(512, col)
        ucuts = [slice(k, k + wide) for k in range(0, col, wide)]
        cuts = list(ucuts)
        half = n_mp // 2
        spans = [(0, half), (half, n_mp)]
        zcuts = []
        for lo, hi in spans:
            step = min(256 * half // (hi - lo), col, feat)
            zcuts.append([slice(k, k + step) for k in range(0, feat, step)])
        if step > 128:
            zcuts[-1][-1:] = [slice(feat - step, feat - step // 2), slice(feat - step // 2, feat)]
        n1 = len(cuts)
        n3 = max(1, col // 1024)
        lhs_rows = -(-users // 16) * 16
        bits = n_mp.bit_length() - 1
        low = max(1, bits - 1)
        block = rows // n_mp
        group = n_mp * n_cand
        shapes = (rows, per_user, users, slots_each, half_width, pool_count, feat, col, cuts, ucuts, zcuts, spans, n3)
        vmem = pl.BlockSpec(memory_space=pltpu.VMEM)
        hbm = pl.BlockSpec(memory_space=pl.ANY)
        dma = pltpu.SemaphoreType.DMA
        crossed, logits = pl.pallas_call(
            make_kernel(n_mp, n_cand, shapes),
            out_shape=(
                pltpu.VMEM((block, col), BF16),
                pltpu.VMEM((1, block), F32),
            ),
            in_specs=[hbm] * 11,
            out_specs=(vmem, vmem),
            scratch_shapes=[
                pltpu.SMEM((1, users), jnp.int32),
                pltpu.VMEM((users, per_user), jnp.int32),
                pltpu.VMEM((1, col), F32),
                pltpu.VMEM((1, feat), F32),
                pltpu.VMEM((1, col), F32),
                pltpu.VMEM((col,), BF16),
                dma((7,)),
                pltpu.VMEM((n_cand, slots_each, half_width), BF16),
                pltpu.VMEM((users, half_width), BF16),
                pltpu.VMEM((users, col), BF16),
                pltpu.VMEM((pool_count, feat), BF16),
                pltpu.VMEM((pool_count, col), BF16),
                pltpu.VMEM((feat, col), BF16),
                pltpu.VMEM((col, feat), BF16),
                pltpu.VMEM((feat, col), BF16),
                pltpu.VMEM((rows, pool_count), BF16),
                pltpu.VMEM((rows, feat), BF16),
                pltpu.VMEM((rows, col), BF16),
                pltpu.VMEM((lhs_rows, feat), BF16),
                pltpu.VMEM((rows, col), F32),
                pltpu.VMEM((rows, col), BF16),
                pltpu.VMEM((low, rows, col), BF16),
                pltpu.VMEM((rows, col), BF16),
                pltpu.VMEM((n_mp, users, col), F32),
                pltpu.VMEM((rows, col), BF16),
                pltpu.VMEM((rows, feat), F32),
                pltpu.VMEM((rows, feat), BF16),
                pltpu.VMEM((2, rows, feat), BF16),
                pltpu.VMEM((2, rows, feat), BF16),
                pltpu.VMEM((rows, feat), BF16),
                pltpu.VMEM((rows, feat), BF16),
                pltpu.VMEM((rows, feat), BF16),
                pltpu.VMEM((rows, feat), BF16),
                pltpu.VMEM((rows, col), F32),
                pltpu.VMEM((rows, col), BF16),
                pltpu.VMEM((n_mp, block, col), BF16),
                pltpu.VMEM((max(rows // 2, 128), 128), F32),
                pltpu.VMEM((len(spans), 1, max(rows // 2, 128)), F32),
                pltpu.VMEM((group, 1, max(rows // 2, 128)), F32),
                dma((4 + n1,)),
                dma((2,)),
                dma((half,)),
                dma((1,)),
                dma((2,)),
                pltpu.SemaphoreType.REGULAR((1,)),
                dma((low,)),
                dma((low, n1)),
                dma((1,)),
                dma((n1,)),
                dma((low,)),
                dma((n1,)),
                dma((1,)),
                dma((len(ucuts),)),
                dma((2,)),
                dma((2, sum(len(part) for part in zcuts))),
                dma((sum(len(part) for part in zcuts),)),
                dma((1,)),
                dma((1,)),
                dma((2,)),
                dma((1,)),
                dma((n3,)),
                dma((2,)),
            ],
            compiler_params=pltpu.CompilerParams(
                collective_id=0, has_side_effects=True, vmem_limit_bytes=67043328 - 3000 * 1024
            ),
        )(
            user_feats, user_slot.reshape(1, -1), cand_pool, cand_ids, first_weight, first_bias.reshape(1, -1),
            second_weight, second_bias.reshape(1, -1), third_weight, third_bias.reshape(1, -1),
            score_weight,
        )
        crossed, logits = pl.pallas_call(
            hand_on,
            out_shape=(
                jax.ShapeDtypeStruct((block, col), BF16),
                jax.ShapeDtypeStruct((1, block), F32),
            ),
            in_specs=[vmem, vmem],
            out_specs=(hbm, hbm),
            scratch_shapes=[dma((2,))],
            compiler_params=pltpu.CompilerParams(vmem_limit_bytes=1024 * 1024),
        )(crossed, logits)
        return crossed, logits.reshape(-1)

    in_specs = (
        P(("groups", "cand"), None),
        P("groups"),
        P("groups", None),
        P("groups", None),
        P("mp", "cand"),
        P("cand"),
        P("cand", "mp"),
        P("mp"),
        P("mp", "cand"),
        P("cand"),
        P("cand"),
    )
    out_specs = (P(("groups", "mp"), "cand"), P(("groups", "mp")))
    return jax.shard_map(body, mesh=mesh, in_specs=in_specs, out_specs=out_specs, check_vma=False)
```
